32 devices in a mesh: member: 4 (over y, x), lat: 8 (over z, core).
Axes of the slice: x: 2, y: 2, z: 4, core: 2. Of those that a mesh axis runs over, the one named last changes fastest.
Arguments:
- state: bfloat16 [4, 64, 720, 128], P('member', 'lat'), may hold values from -6 to 6
- conv_weight: bfloat16 [9, 128, 128], replicated, may hold values from -0.1875 to 0.1875
- legendre: bfloat16 [64, 64, 64], P('lat'), may hold values from -0.75 to 0.75
- quad_weight: float32 [64], replicated, may hold values from 0.5 to 2
- spectral_gain: float32 [2, 64, 128], replicated, may hold values from -4 to 4
- project_weight: float32 [128, 16], replicated, may hold values from -0.5 to 0.5
- target: bfloat16 [16, 64, 720], P(None, 'lat'), may hold values from -10 to 10
Outputs:
- field_grad: float32 [4, 16, 64, 720], P('member', None, 'lat')
The draws below stay inside these ranges and needn't reach their ends.
All inputs are finite; a program needn't handle non-finite values.
Results may differ from the reference program's by a relative error of at most 0.0088.
Values may be sent and summed in bfloat16 or wider, within the bound.
A program may use at most 64 MiB of HBM per device.

```python
import math
import jax
import jax.numpy as jnp
from jax import lax

NLON = 720
C = 128
FIELDS = 16
MODES = 64
NLAT = 64
MEMBERS = 4


def level_of(key, shape, pieces, low, high):
    loudness = 1.0
    for axis_at, parts in pieces:
        heights = jax.random.uniform(jax.random.fold_in(jax.random.fold_in(key, 6), axis_at), (parts,), jnp.float32, low / len(pieces), high / len(pieces))
        loudness = loudness * jnp.repeat(jnp.exp(heights), shape[axis_at] // parts).reshape((-1,) + (1,) * (len(shape) - 1 - axis_at))
    return loudness


def gaussian(key, shape, width, bound, shards=(), kind=jnp.bfloat16):
    result = jax.random.normal(key, shape, jnp.float32) * width
    if len(shards) > 0:
        result = level_of(key, shape, shards, -0.22, 0.18) * result
    return jnp.clip(result, min=-bound, max=bound).astype(kind)


def setup_inputs(seed: int = 0) -> dict:
    keys = jax.random.split(jax.random.key(seed), 8)
    return {
        "state": gaussian(keys[0], (MEMBERS, NLAT, NLON, C), 1.0, 6.0, ((0, 4), (1, 8))),
        "conv_weight": gaussian(keys[1], (9, C, C), (9 * C) ** -0.5, 0.1875),
        "legendre": gaussian(keys[2], (MODES, MODES, NLAT), NLAT ** -0.5, 0.75, ((0, 8),)),
        "quad_weight": jnp.clip(jnp.exp(jax.random.uniform(keys[3], (NLAT,), jnp.float32, math.log(0.5), math.log(2.0))), 0.5, 2.0),
        "spectral_gain": gaussian(keys[4], (2, MODES, C), 1.0, 4.0, (), jnp.float32),
        "project_weight": gaussian(keys[5], (C, FIELDS), C ** -0.5, 0.5, (), jnp.float32),
        "target": gaussian(keys[6], (FIELDS, NLAT, NLON), 2.0, 10.0, ((1, 8),)),
    }


def dft_table(nlon, modes):
    lon = jnp.arange(nlon, dtype=jnp.int32)
    wave = jnp.arange(modes, dtype=jnp.int32)
    phase = lon[:, None] * wave[None, :] % nlon
    angle = phase.astype(jnp.float32) * (2.0 * jnp.pi / nlon)
    table = jnp.concatenate([jnp.cos(angle), -jnp.sin(angle)], axis=1) / jnp.sqrt(jnp.float32(nlon))
    return table.astype(jnp.bfloat16)

def smooth(diff):
    return diff / jnp.sqrt(diff * diff + 0.25)

def reference(state, conv_weight, legendre, quad_weight, spectral_gain, project_weight, target):
    table = dft_table(NLON, MODES).astype(jnp.float32)
    wtable = (legendre.astype(jnp.float32) * quad_weight[None, None, :]).astype(jnp.bfloat16).astype(jnp.float32)
    legend = legendre.astype(jnp.float32)
    weights = conv_weight.astype(jnp.float32)
    gain_re = spectral_gain[0]
    gain_im = spectral_gain[1]

    def member_field(field):
        padded = jnp.pad(field, ((4, 4), (0, 0), (0, 0))).astype(jnp.float32)
        conv = jnp.zeros((NLAT, NLON, C), jnp.float32)
        for shift in range(9):
            conv = conv + jnp.einsum('anc,cd->and', padded[shift:shift + NLAT], weights[shift])
        mixed = (field.astype(jnp.float32) + jax.nn.silu(conv)).astype(jnp.bfloat16)
        spectrum = jnp.einsum('anc,nk->akc', mixed.astype(jnp.float32), table).astype(jnp.bfloat16)
        spectrum = spectrum.reshape(NLAT, 2, MODES, C).astype(jnp.float32)
        coef = jnp.einsum('mla,armc->mlrc', wtable, spectrum)
        real_part = coef[:, :, 0] * gain_re[None] - coef[:, :, 1] * gain_im[None]
        imag_part = coef[:, :, 0] * gain_im[None] + coef[:, :, 1] * gain_re[None]
        filtered = jnp.stack([real_part, imag_part], axis=2).astype(jnp.bfloat16).astype(jnp.float32)
        back = jnp.einsum('mla,mlrc->armc', legend, filtered).astype(jnp.bfloat16)
        back = back.reshape(NLAT, 2 * MODES, C).astype(jnp.float32)
        synth = jnp.einsum('akc,nk->anc', back, table)
        total = mixed.astype(jnp.float32) + synth
        projected = jnp.einsum('anc,cf->fan', total, project_weight, precision=lax.Precision.HIGHEST)
        return projected.astype(jnp.bfloat16)
    projected = lax.map(member_field, state).astype(jnp.float32)
    observed = target.astype(jnp.float32)

    def member_grad(own):
        pair = lax.optimization_barrier(jnp.sum(smooth(own[None] - projected), axis=0))
        return smooth(own - observed) - pair / (MEMBERS - 1)
    return lax.map(member_grad, projected)
```

```python
import functools
import jax
import jax.numpy as jnp
import numpy as np
from jax import lax
from jax.experimental import pallas as pl
from jax.experimental.pallas import tpu as pltpu
from jax.sharding import PartitionSpec as P

MESH = pl.DeviceIdType.MESH
HALF = 4
F32 = jnp.float32
BF16 = jnp.bfloat16


def dft_table(nlon, modes, bands):
    phase = np.arange(nlon)[:, None] * np.arange(modes)[None, :] % nlon
    angle = phase * (2.0 * np.pi / nlon)
    table = np.stack([np.cos(angle), -np.sin(angle)], axis=1) / np.sqrt(nlon)
    table = table.reshape(nlon, 2, bands, modes // bands).swapaxes(1, 2)
    return jnp.asarray(table.reshape(nlon, 2 * modes).T.astype(np.float32), BF16)


def dot(a, b, contract=((1,), (0,))):
    return lax.dot_general(a, b, (contract, ((), ())), preferred_element_type=F32)


def smooth(diff):
    return diff * lax.rsqrt(diff * diff + 0.25)


def pick(shape, axis, cond):
    return jnp.where(cond(lax.broadcasted_iota(jnp.int32, shape, axis)), 1.0, 0.0)


def kernel(
    members,
    bands,
    state,
    conv_hbm,
    leg_hbm,
    quad_hbm,
    gain_hbm,
    proj_hbm,
    target_hbm,
    table_hbm,
    out_hbm,
    rows,
    conv_w,
    leg,
    quad,
    gain,
    proj,
    target,
    table,
    toeplitz,
    mixed,
    spec,
    banded,
    spread,
    wtable,
    legx,
    filt,
    filtw,
    wrep,
    drep,
    directs,
    narrowf,
    narrow,
    everyone,
    grads,
    load_sems,
    halo_sems,
    send_sems,
    spec_sems,
    direct_sems,
    back_sem,
    out_sem,
    lat_sems,
    member_sems,
):
    member, band = lax.axis_index("member"), lax.axis_index("lat")
    _, lat_rows, nlon, chans = state.shape
    pairs = lat_rows // 2
    nlat = bands * lat_rows
    mb, degrees = leg.shape[0], leg.shape[1]
    wide = 2 * mb
    fields = proj.shape[0]
    fa = fields * lat_rows
    has_low, has_high = band > 0, band < bands - 1

    barrier = pltpu.get_barrier_semaphore()
    hops = [1 << i for i in range((members - 1).bit_length())]

    def greet_lat(sem, dist):
        @pl.when(band >= dist)
        def _():
            pl.semaphore_signal(sem, 1, device_id=(member, band - dist), device_id_type=MESH)

        @pl.when(band + dist < bands)
        def _():
            pl.semaphore_signal(sem, 1, device_id=(member, band + dist), device_id_type=MESH)

    def count_lat(dist):
        return (band >= dist).astype(jnp.int32) + (band + dist < bands).astype(jnp.int32)

    greet_lat(barrier, 1)
    for hop in hops:
        pl.semaphore_signal(barrier, 1, device_id=(member ^ hop, band), device_id_type=MESH)
    loads = [
        (state.at[0], rows.at[pl.ds(HALF, lat_rows)]),
        (conv_hbm, conv_w),
        (table_hbm, table),
        (leg_hbm, leg),
        (quad_hbm, quad),
        (gain_hbm, gain),
        (proj_hbm, proj),
        (target_hbm, target),
    ]
    loads = [pltpu.make_async_copy(a, b, load_sems.at[i]) for i, (a, b) in enumerate(loads)]
    for copy in loads:
        copy.start()
    pl.semaphore_wait(barrier, count_lat(1) + len(hops))

    rounds = []
    known = 1
    while known < bands - 1:
        rounds.append(known)
        known *= 2

    def round_signal(i):
        if i < len(rounds):
            greet_lat(lat_sems.at[i], rounds[i])
        elif i < len(rounds) + len(hops):
            j = i - len(rounds)
            pl.semaphore_signal(
                member_sems.at[j], 1, device_id=(member ^ hops[j], band), device_id_type=MESH
            )

    def round_wait(i):
        if i < len(rounds):
            pl.semaphore_wait(lat_sems.at[i], count_lat(rounds[i]))
        elif i < len(rounds) + len(hops):
            pl.semaphore_wait(member_sems.at[i - len(rounds)], 1)

    def step_round(i):
        round_wait(i)
        round_signal(i + 1)

    round_signal(0)

    def halo(up, far):
        if up:
            src = lat_rows - 2 - 2 * far
            dst = HALF - 2 - 2 * far
            peer = band + 1
        else:
            src = 2 * far
            dst = HALF + lat_rows + 2 * far
            peer = band - 1
        sem = 2 * (0 if up else 1) + far
        return pltpu.make_async_remote_copy(
            state.at[0, pl.ds(src, 2)],
            rows.at[pl.ds(dst, 2)],
            send_sems.at[sem],
            halo_sems.at[sem],
            device_id=(member, peer),
            device_id_type=MESH,
        )

    for far in (0, 1):

        @pl.when(has_high)
        def _():
            halo(True, far).start()

        @pl.when(has_low)
        def _():
            halo(False, far).start()

    @pl.when(jnp.logical_not(has_low))
    def _():
        rows[0:HALF] = jnp.zeros((HALF, nlon, chans), BF16)

    @pl.when(jnp.logical_not(has_high))
    def _():
        rows[HALF + lat_rows :] = jnp.zeros((HALF, nlon, chans), BF16)

    def halo_wait(low, far):
        @pl.when(has_low if low else has_high)
        def _():
            halo(low, far).wait_recv()

    loads[1].wait()
    taps = conv_w.shape[0]
    for d in range(HALF + 1):
        for e in (0, 1):
            for f in (0, 1):
                tap = 2 * d + e - f
                w = conv_w[tap] if 0 <= tap < taps else jnp.zeros((chans, chans), BF16)
                at = (2 * d + e) * chans
                toeplitz[at : at + chans, f * chans : (f + 1) * chans] = w
    step_round(0)

    even = band % 2 == 0

    def pair_of(t):
        return jnp.where(even, pairs - 1 - t, t)

    def convolve(t):
        p = pair_of(t)
        window = [rows[2 * p + j] for j in range(2 * HALF + 2)]
        conv = dot(jnp.concatenate(window, axis=1), toeplitz[...])
        own = jnp.concatenate([rows[2 * p + HALF], rows[2 * p + HALF + 1]], axis=1)
        half = conv * 0.5
        mixed[p] = (own.astype(F32) + half + half * jnp.tanh(half)).astype(BF16)

    def transform(t):
        p = pair_of(t)
        s = dot(table[...], mixed[p]).astype(BF16)
        for e in (0, 1):
            spec[p, :, e] = s[:, e * chans : (e + 1) * chans].reshape(bands, wide, chans)

    def send_spec(t):
        p = pair_of(t)

        @pl.loop(1, bands)
        def _(k):
            peer = (band + k) % bands
            pltpu.make_async_remote_copy(
                spec.at[p, peer], banded.at[band, p], send_sems.at[4], spec_sems.at[t],
                device_id=(member, peer), device_id_type=MESH,
            ).start()

        pltpu.make_async_copy(spec.at[p, band], banded.at[band, p], spec_sems.at[t]).start()

    loads[0].wait()

    @pl.when(even)
    def _():
        halo_wait(False, 0)
        halo_wait(False, 1)

    @pl.when(jnp.logical_not(even))
    def _():
        halo_wait(True, 0)
        halo_wait(True, 1)

    convolve(0)
    step_round(1)
    loads[2].wait()
    transform(0)
    convolve(1)
    step_round(2)
    transform(1)
    for i in range(3, len(rounds)):
        step_round(i)

    for copy in loads[3:]:
        copy.wait()
    wtable[...] = (leg[...].astype(F32) * quad[...]).astype(BF16)
    flat_leg = leg[...].reshape(mb * degrees, nlat)

    @pl.loop(0, bands)
    def _(s):
        at = lax.broadcasted_iota(jnp.int32, (nlat, fa), 0)
        lane = lax.broadcasted_iota(jnp.int32, (nlat, fa), 1)
        onehot = jnp.where(at == s * lat_rows + lane % lat_rows, 1.0, 0.0).astype(BF16)
        legx[s] = dot(flat_leg, onehot).astype(BF16)

    high = proj[...].astype(BF16)
    low = (proj[...] - high.astype(F32)).astype(BF16)
    r0 = lax.broadcasted_iota(jnp.int32, (fa, fields), 0)
    r1 = lax.broadcasted_iota(jnp.int32, (fa, fields), 1)
    repeat = jnp.where(r0 // lat_rows == r1, 1.0, 0.0).astype(BF16)
    arow = lax.broadcasted_iota(jnp.int32, (fa, chans), 0) % lat_rows
    for i, part in enumerate((high, low)):
        wide_rows = dot(repeat, part)
        wrep[i * chans : (i + 1) * chans, :] = wide_rows.T.astype(BF16)
        for a in range(lat_rows):
            drep[i * fa : (i + 1) * fa, a * chans : (a + 1) * chans] = jnp.where(
                arow == a, wide_rows, 0.0
            ).astype(BF16)

    @pl.when(even)
    def _():
        halo_wait(True, 0)

    @pl.when(jnp.logical_not(even))
    def _():
        halo_wait(False, 0)

    for t in range(2, pairs - 1):
        convolve(t)
        transform(t)
    for i in range(max(3, len(rounds)), len(rounds) + len(hops)):
        step_round(i)

    @pl.when(even)
    def _():
        halo_wait(True, 1)

    @pl.when(jnp.logical_not(even))
    def _():
        halo_wait(False, 1)

    for t in range(pairs - 1):
        send_spec(t)
    convolve(pairs - 1)
    transform(pairs - 1)
    send_spec(pairs - 1)

    fine = dot(
        drep[...], jnp.concatenate([mixed[p] for p in range(pairs)], axis=1), ((1,), (1,))
    )
    directs[member] = (fine[:fa] + fine[fa:]).astype(BF16)

    @pl.loop(1, members)
    def _(k):
        peer = (member + k) % members
        pltpu.make_async_remote_copy(
            directs.at[member], directs.at[member], send_sems.at[5], direct_sems.at[0],
            device_id=(peer, band), device_id_type=MESH,
        ).start()

    for t in range(pairs):
        pltpu.make_async_copy(banded.at[:, t], banded.at[:, t], spec_sems.at[t]).wait()
    spread[...] = banded[...].astype(F32).reshape(nlat * wide, chans)
    gain_re, gain_im = gain[0], gain[1]
    for m in range(mb):
        re = spread[pl.ds(m, nlat, stride=wide), :]
        im = spread[pl.ds(mb + m, nlat, stride=wide), :]
        coef = dot(wtable[m], jnp.concatenate([re, im], axis=1).astype(BF16))
        c0, c1 = coef[:, :chans], coef[:, chans:]
        for r, part in enumerate((c0 * gain_re - c1 * gain_im, c0 * gain_im + c1 * gain_re)):
            part = part.astype(BF16)
            filt[m, r] = jnp.concatenate([part, part], axis=1)
    filtw[...] = dot(filt[...].reshape(mb * 2 * degrees, 2 * chans), wrep[...]).reshape(
        mb, 2, degrees, fa
    )

    @pl.loop(0, bands)
    def _(s):
        for m in range(mb):
            lx = legx[s, m * degrees : (m + 1) * degrees, :].astype(F32)
            for r in (0, 1):
                at = r * mb + m
                narrowf[s, at : at + 1, :] = jnp.sum(lx * filtw[m, r], axis=0, keepdims=True)

    narrow[...] = narrowf[...].astype(BF16)

    count = members * bands
    me = member * bands + band

    @pl.loop(1, count)
    def _(k):
        peer = (me + k) % count
        pltpu.make_async_remote_copy(
            narrow.at[peer % bands], everyone.at[me], send_sems.at[6], back_sem.at[0],
            device_id=(peer // bands, peer % bands), device_id_type=MESH,
        ).start()

    pltpu.make_async_copy(narrow.at[band], everyone.at[me], back_sem.at[0]).start()
    sent = directs.at[pl.ds(0, members - 1)]
    pltpu.make_async_copy(sent, sent, direct_sems.at[0]).wait()
    pltpu.make_async_copy(everyone, everyone, back_sem.at[0]).wait()

    def projected(j):
        k = everyone[pl.ds(j * bands, bands)].reshape(bands * wide, fa)
        synth = dot(k, table[...], ((0,), (0,)))
        return (directs[j].astype(F32) + synth).astype(BF16).astype(F32)

    own = projected(member)
    observed = target[...].astype(F32).reshape(fa, nlon)
    grads[...] = smooth(own - observed)

    @pl.loop(1, members)
    def _(k):
        grads[...] -= smooth(own - projected((member + k) % members)) * (1.0 / (members - 1))

    done = pltpu.make_async_copy(grads, out_hbm, out_sem.at[0])
    done.start()

    for far in (0, 1):

        @pl.when(has_high)
        def _():
            halo(True, far).wait_send()

        @pl.when(has_low)
        def _():
            halo(False, far).wait_send()

    sent = banded.at[pl.ds(0, bands - 1)]
    pltpu.make_async_copy(sent, sent, send_sems.at[4]).wait()
    sent = directs.at[pl.ds(0, members - 1)]
    pltpu.make_async_copy(sent, sent, send_sems.at[5]).wait()

    sent = everyone.at[pl.ds(0, count - 1)]
    pltpu.make_async_copy(sent, sent, send_sems.at[6]).wait()

    done.wait()


def local(state, conv_weight, legendre, quad_weight, spectral_gain, project_weight, target):
    _, lat_rows, nlon, chans = state.shape
    mb, degrees, nlat = legendre.shape
    members, bands = lax.axis_size("member"), lax.axis_size("lat")
    fields = project_weight.shape[1]
    fa, wide, pairs = fields * lat_rows, 2 * mb, lat_rows // 2
    table = dft_table(nlon, mb * bands, bands)
    vmem = pltpu.VMEM
    dma, plain = pltpu.SemaphoreType.DMA, pltpu.SemaphoreType.REGULAR
    out = pl.pallas_call(
        functools.partial(kernel, members, bands),
        out_shape=jax.ShapeDtypeStruct((fa, nlon), F32),
        in_specs=[pl.BlockSpec(memory_space=pl.ANY)] * 8,
        out_specs=pl.BlockSpec(memory_space=pl.ANY),
        scratch_shapes=[
            vmem((lat_rows + 2 * HALF, nlon, chans), BF16),
            vmem(conv_weight.shape, BF16),
            vmem(legendre.shape, BF16),
            vmem((1, nlat), F32),
            vmem(spectral_gain.shape, F32),
            vmem((fields, chans), F32),
            vmem(target.shape, BF16),
            vmem(table.shape, BF16),
            vmem(((2 * HALF + 2) * chans, 2 * chans), BF16),
            vmem((pairs, nlon, 2 * chans), BF16),
            vmem((pairs, bands, 2, wide, chans), BF16),
            vmem((bands, pairs, 2, wide, chans), BF16),
            vmem((nlat * wide, chans), F32),
            vmem(legendre.shape, BF16),
            vmem((bands, mb * degrees, fa), BF16),
            vmem((mb, 2, degrees, 2 * chans), BF16),
            vmem((mb, 2, degrees, fa), F32),
            vmem((2 * chans, fa), BF16),
            vmem((2 * fa, lat_rows * chans), BF16),
            vmem((members, fa, nlon), BF16),
            vmem((bands, wide, fa), F32),
            vmem((bands, wide, fa), BF16),
            vmem((members * bands, wide, fa), BF16),
            vmem((fa, nlon), F32),
            dma((8,)),
            dma((4,)),
            dma((7,)),
            dma((pairs,)),
            dma((1,)),
            dma((1,)),
            dma((1,)),
            plain((max(1, (bands - 1).bit_length()),)),
            plain((max(1, (members - 1).bit_length()),)),
        ],
        compiler_params=pltpu.CompilerParams(
            collective_id=0, has_side_effects=True, vmem_limit_bytes=60 * 1024 * 1024
        ),
    )(
        state,
        conv_weight,
        legendre,
        quad_weight.reshape(1, nlat),
        spectral_gain,
        project_weight.T,
        target,
        table,
    )
    return out.reshape(1, fields, lat_rows, nlon)


def solution(mesh):
    return jax.shard_map(
        local,
        mesh=mesh,
        in_specs=(
            P("member", "lat", None, None),
            P(),
            P("lat", None, None),
            P(),
            P(),
            P(),
            P(None, "lat", None),
        ),
        out_specs=P("member", None, "lat", None),
        check_vma=False,
    )
```

```python
import functools
import jax
import jax.numpy as jnp
import numpy as np
from jax import lax
from jax.experimental import pallas as pl
from jax.experimental.pallas import tpu as pltpu
from jax.sharding import PartitionSpec as P

MESH = pl.DeviceIdType.MESH
HALF = 4
LANES = 128
F32 = jnp.float32
BF16 = jnp.bfloat16


def dft_table(nlon, modes, bands):
    phase = np.arange(nlon)[:, None] * np.arange(modes)[None, :] % nlon
    angle = phase * (2.0 * np.pi / nlon)
    table = np.stack([np.cos(angle), -np.sin(angle)], axis=1) / np.sqrt(nlon)
    table = table.reshape(nlon, 2, bands, modes // bands).swapaxes(1, 2)
    return jnp.asarray(table.reshape(nlon, 2 * modes).T.astype(np.float32), BF16)


def dot(a, b, contract=((1,), (0,))):
    return lax.dot_general(a, b, (contract, ((), ())), preferred_element_type=F32)


def smooth(diff):
    return diff * lax.rsqrt(diff * diff + 0.25)


def kernel(
    members,
    bands,
    state,
    conv_hbm,
    leg_hbm,
    quad_hbm,
    gain_hbm,
    proj_hbm,
    target_hbm,
    table_hbm,
    out,
    rows,
    conv_w,
    leg,
    quad,
    gain,
    proj,
    target,
    table,
    toeplitz,
    mixed,
    spec,
    banded,
    spread,
    wtable,
    legx,
    filt,
    filtw,
    wrep,
    drep,
    directs,
    narrowf,
    narrow,
    everyone,
    observed,
    own_rows,
    mine,
    load_sems,
    halo_sems,
    send_sems,
    spec_sems,
    direct_sems,
    back_sems,
    lat_sems,
    member_sems,
):
    member, band = lax.axis_index("member"), lax.axis_index("lat")
    _, lat_rows, nlon, chans = state.shape
    pairs = lat_rows // 2
    nlat = bands * lat_rows
    mb, degrees = leg.shape[0], leg.shape[1]
    wide = 2 * mb
    fields = proj.shape[0]
    fa = fields * lat_rows
    lanes = [slice(i, min(i + LANES, nlon)) for i in range(0, nlon, LANES)]
    has_low, has_high = band > 0, band < bands - 1

    barrier = pltpu.get_barrier_semaphore()
    hops = [1 << i for i in range((members - 1).bit_length())]

    def greet_lat(sem, dist):
        @pl.when(band >= dist)
        def _():
            pl.semaphore_signal(sem, 1, device_id=(member, band - dist), device_id_type=MESH)

        @pl.when(band + dist < bands)
        def _():
            pl.semaphore_signal(sem, 1, device_id=(member, band + dist), device_id_type=MESH)

    def count_lat(dist):
        return (band >= dist).astype(jnp.int32) + (band + dist < bands).astype(jnp.int32)

    greet_lat(barrier, 1)
    for hop in hops:
        pl.semaphore_signal(barrier, 1, device_id=(member ^ hop, band), device_id_type=MESH)
    loads = [
        (state.at[0], rows.at[pl.ds(HALF, lat_rows)]),
        (conv_hbm, conv_w),
        (table_hbm, table),
        (leg_hbm, leg),
        (quad_hbm, quad),
        (gain_hbm, gain),
        (proj_hbm, proj),
        (target_hbm, target),
    ]
    loads = [pltpu.make_async_copy(a, b, load_sems.at[i]) for i, (a, b) in enumerate(loads)]
    for copy in loads:
        copy.start()
    pl.semaphore_wait(barrier, count_lat(1) + len(hops))

    rounds = []
    for i, hop in enumerate(hops[1:]):
        rounds.append((member_sems.at[i], hop, None))
    known = 1
    while known < bands - 1:
        rounds.append((lat_sems.at[len(rounds) - len(hops) + 1], None, known))
        known *= 2

    def round_signal(i):
        if i < len(rounds):
            sem, hop, dist = rounds[i]
            if hop is None:
                greet_lat(sem, dist)
            else:
                pl.semaphore_signal(sem, 1, device_id=(member ^ hop, band), device_id_type=MESH)

    def step_round(i):
        if i < len(rounds):
            sem, hop, dist = rounds[i]
            pl.semaphore_wait(sem, 1 if hop is not None else count_lat(dist))
            round_signal(i + 1)

    round_signal(0)

    def halo(up, far):
        if up:
            src = lat_rows - 2 - 2 * far
            dst = HALF - 2 - 2 * far
            peer = band + 1
        else:
            src = 2 * far
            dst = HALF + lat_rows + 2 * far
            peer = band - 1
        sem = 2 * (0 if up else 1) + far
        return pltpu.make_async_remote_copy(
            state.at[0, pl.ds(src, 2)],
            rows.at[pl.ds(dst, 2)],
            send_sems.at[sem],
            halo_sems.at[sem],
            device_id=(member, peer),
            device_id_type=MESH,
        )

    even = band % 2 == 0

    @pl.when(even & has_low)
    def _():
        halo(False, 0).start()
        halo(False, 1).start()

    @pl.when(has_high)
    def _():
        halo(True, 0).start()
        halo(True, 1).start()

    @pl.when(jnp.logical_not(even) & has_low)
    def _():
        halo(False, 0).start()
        halo(False, 1).start()

    @pl.when(jnp.logical_not(has_low))
    def _():
        rows[0:HALF] = jnp.zeros((HALF, nlon, chans), BF16)

    @pl.when(jnp.logical_not(has_high))
    def _():
        rows[HALF + lat_rows :] = jnp.zeros((HALF, nlon, chans), BF16)

    def halo_wait(low, far):
        @pl.when(has_low if low else has_high)
        def _():
            halo(low, far).wait_recv()

    loads[1].wait()
    taps = conv_w.shape[0]
    for d in range(HALF + 1):
        for e in (0, 1):
            for f in (0, 1):
                tap = 2 * d + e - f
                w = conv_w[tap] if 0 <= tap < taps else jnp.zeros((chans, chans), BF16)
                at = (2 * d + e) * chans
                toeplitz[at : at + chans, f * chans : (f + 1) * chans] = w
    def pair_of(t):
        return jnp.where(even, pairs - 1 - t, t)

    def convolve(t):
        p = pair_of(t)
        window = [rows[2 * p + j] for j in range(2 * HALF + 2)]
        conv = dot(jnp.concatenate(window, axis=1), toeplitz[...])
        own = jnp.concatenate([rows[2 * p + HALF], rows[2 * p + HALF + 1]], axis=1)
        half = conv * 0.5
        mixed[p] = (own.astype(F32) + half + half * jnp.tanh(half)).astype(BF16)

    def transform(t):
        p = pair_of(t)
        s = dot(table[...], mixed[p]).astype(BF16)
        for e in (0, 1):
            spec[p, :, e] = s[:, e * chans : (e + 1) * chans].reshape(bands, wide, chans)

    def send_spec(t):
        p = pair_of(t)

        def to(peer):
            pltpu.make_async_remote_copy(
                spec.at[p, peer], banded.at[band, p], send_sems.at[4], spec_sems.at[t],
                device_id=(member, peer), device_id_type=MESH,
            ).start()

        @pl.loop(1, bands)
        def _(k):
            dist = bands - k

            @pl.when(band + dist < bands)
            def _():
                to(band + dist)

            @pl.when(band >= dist)
            def _():
                to(band - dist)

        pltpu.make_async_copy(spec.at[p, band], banded.at[band, p], spec_sems.at[t]).start()

    def direct(t):
        p = pair_of(t)
        fine = dot(drep[...], mixed[p], ((1,), (1,)))
        half = 2 * fields
        at = pl.ds(p * half, half)
        directs[member, at] = (fine[:half] + fine[half:]).astype(BF16)

        @pl.loop(1, members)
        def _(k):
            part = directs.at[member, at]
            pltpu.make_async_remote_copy(
                part, part, send_sems.at[5], direct_sems.at[0],
                device_id=((member + k) % members, band), device_id_type=MESH,
            ).start()

    loads[6].wait()
    high = proj[...].astype(BF16)
    low = (proj[...] - high.astype(F32)).astype(BF16)
    r0 = lax.broadcasted_iota(jnp.int32, (fa, fields), 0) % fields
    r1 = lax.broadcasted_iota(jnp.int32, (fa, fields), 1)
    tile = jnp.where(r0 == r1, 1.0, 0.0).astype(BF16)
    for i, part in enumerate((high, low)):
        wrep[i * chans : (i + 1) * chans, :] = dot(tile, part).T.astype(BF16)
        for e in (0, 1):
            at = (2 * i + e) * fields
            drep[at : at + fields, e * chans : (e + 1) * chans] = part
            drep[at : at + fields, (1 - e) * chans : (2 - e) * chans] = jnp.zeros_like(part)
    step_round(0)

    loads[0].wait()

    @pl.when(even)
    def _():
        halo_wait(False, 0)
        halo_wait(False, 1)

    @pl.when(jnp.logical_not(even))
    def _():
        halo_wait(True, 0)
        halo_wait(True, 1)

    convolve(0)
    step_round(1)
    loads[2].wait()
    transform(0)
    direct(0)
    convolve(1)
    step_round(2)
    transform(1)
    direct(1)

    for i in (3, 4, 5, 7):
        loads[i].wait()
    wtable[...] = (leg[...].astype(F32) * quad[...]).astype(BF16)
    flat_leg = leg[...].reshape(mb * degrees, nlat)

    @pl.loop(0, bands)
    def _(s):
        at = lax.broadcasted_iota(jnp.int32, (nlat, fa), 0)
        lane = lax.broadcasted_iota(jnp.int32, (nlat, fa), 1)
        onehot = jnp.where(at == s * lat_rows + lane // fields, 1.0, 0.0).astype(BF16)
        legx[s] = dot(flat_leg, onehot).astype(BF16)

    for i in range(3, len(rounds)):
        step_round(i)

    @pl.when(even)
    def _():
        halo_wait(True, 0)

    @pl.when(jnp.logical_not(even))
    def _():
        halo_wait(False, 0)

    send_spec(0)
    send_spec(1)
    for t in range(2, pairs - 1):
        convolve(t)
        transform(t)
        send_spec(t)
        direct(t)

    @pl.when(even)
    def _():
        halo_wait(True, 1)

    @pl.when(jnp.logical_not(even))
    def _():
        halo_wait(False, 1)

    convolve(pairs - 1)
    transform(pairs - 1)
    send_spec(pairs - 1)
    direct(pairs - 1)
    for i, at in enumerate(lanes):
        width = at.stop - at.start
        own_rows[i, :, :width] = target[:, :, at].astype(F32).reshape(fa, width)
        for a in range(lat_rows):
            rows_of = own_rows[i, pl.ds(a, fields, stride=lat_rows), :]
            observed[a * fields : (a + 1) * fields, at] = rows_of[:, :width]

    for t in range(pairs):
        pltpu.make_async_copy(banded.at[:, t], banded.at[:, t], spec_sems.at[t]).wait()
    spread[...] = banded[...].astype(F32).reshape(nlat * wide, chans)
    gain_re, gain_im = gain[0], gain[1]
    for m in range(mb):
        re = spread[pl.ds(m, nlat, stride=wide), :]
        im = spread[pl.ds(mb + m, nlat, stride=wide), :]
        coef = dot(wtable[m], jnp.concatenate([re, im], axis=1).astype(BF16))
        c0, c1 = coef[:, :chans], coef[:, chans:]
        for r, part in enumerate((c0 * gain_re - c1 * gain_im, c0 * gain_im + c1 * gain_re)):
            part = part.astype(BF16)
            filt[m, r] = jnp.concatenate([part, part], axis=1)
    filtw[...] = dot(filt[...].reshape(mb * 2 * degrees, 2 * chans), wrep[...]).reshape(
        mb, 2, degrees, fa
    )

    def strip(s):
        for m in range(mb):
            lx = legx[s, m * degrees : (m + 1) * degrees, :].astype(F32)
            for r in (0, 1):
                at = r * mb + m
                narrowf[s, at : at + 1, :] = jnp.sum(lx * filtw[m, r], axis=0, keepdims=True)
        narrow[s] = narrowf[s].astype(BF16)

    me = member * bands + band

    def back(k, s):
        pltpu.make_async_remote_copy(
            narrow.at[s], everyone.at[me], send_sems.at[6], back_sems.at[member],
            device_id=((member + k) % members, s), device_id_type=MESH,
        ).start()

    @pl.loop(1, bands)
    def _(i):
        s = jnp.where(band < bands // 2, bands - i, i - 1)
        s = jnp.where(jnp.where(band < bands // 2, s <= band, s >= band), jnp.where(band < bands // 2, s - 1, s + 1), s)
        strip(s)

        @pl.loop(0, members)
        def _(k):
            back(k, s)

    strip(band)

    @pl.loop(1, members)
    def _(k):
        back(k, band)

    pltpu.make_async_copy(narrow.at[band], everyone.at[me], back_sems.at[member]).start()

    def back_wait(j):
        arrived = everyone.at[pl.ds(j * bands, bands)]
        pltpu.make_async_copy(arrived, arrived, back_sems.at[j]).wait()

    def projected(j):
        k = everyone[pl.ds(j * bands, bands)].reshape(bands * wide, fa)
        synth = dot(k, table[...], ((0,), (0,)))
        return (directs[j].astype(F32) + synth).astype(BF16).astype(F32)

    back_wait(member)
    own = projected(member)
    observed[...] = smooth(own - observed[...])
    mine[...] = own
    sent = directs.at[pl.ds(0, members - 1)]
    pltpu.make_async_copy(sent, sent, direct_sems.at[0]).wait()

    @pl.loop(1, members)
    def _(k):
        j = (member + k) % members
        back_wait(j)
        observed[...] -= smooth(mine[...] - projected(j)) * (1.0 / (members - 1))

    for i, at in enumerate(lanes):
        width = at.stop - at.start
        own_rows[i, :, :width] = observed[:, at]
        for f in range(fields):
            rows_of = own_rows[i, pl.ds(f, lat_rows, stride=fields), :]
            out[f * lat_rows : (f + 1) * lat_rows, at] = rows_of[:, :width]

    for far in (0, 1):

        @pl.when(has_high)
        def _():
            halo(True, far).wait_send()

        @pl.when(has_low)
        def _():
            halo(False, far).wait_send()

    sent = banded.at[pl.ds(0, bands - 1)]
    pltpu.make_async_copy(sent, sent, send_sems.at[4]).wait()
    sent = directs.at[pl.ds(0, members - 1)]
    pltpu.make_async_copy(sent, sent, send_sems.at[5]).wait()

    sent = everyone.at[pl.ds(0, members * bands - 1)]
    pltpu.make_async_copy(sent, sent, send_sems.at[6]).wait()


def local(state, conv_weight, legendre, quad_weight, spectral_gain, project_weight, target):
    _, lat_rows, nlon, chans = state.shape
    mb, degrees, nlat = legendre.shape
    members, bands = lax.axis_size("member"), lax.axis_size("lat")
    fields = project_weight.shape[1]
    fa, wide, pairs = fields * lat_rows, 2 * mb, lat_rows // 2
    table = dft_table(nlon, mb * bands, bands)
    vmem = pltpu.VMEM
    dma, plain = pltpu.SemaphoreType.DMA, pltpu.SemaphoreType.REGULAR
    out = pl.pallas_call(
        functools.partial(kernel, members, bands),
        out_shape=pltpu.VMEM((fa, nlon), F32),
        in_specs=[pl.BlockSpec(memory_space=pl.ANY)] * 8,
        out_specs=pl.BlockSpec(memory_space=pltpu.VMEM),
        scratch_shapes=[
            vmem((lat_rows + 2 * HALF, nlon, chans), BF16),
            vmem(conv_weight.shape, BF16),
            vmem(legendre.shape, BF16),
            vmem((1, nlat), F32),
            vmem(spectral_gain.shape, F32),
            vmem((fields, chans), F32),
            vmem(target.shape, BF16),
            vmem(table.shape, BF16),
            vmem(((2 * HALF + 2) * chans, 2 * chans), BF16),
            vmem((pairs, nlon, 2 * chans), BF16),
            vmem((pairs, bands, 2, wide, chans), BF16),
            vmem((bands, pairs, 2, wide, chans), BF16),
            vmem((nlat * wide, chans), F32),
            vmem(legendre.shape, BF16),
            vmem((bands, mb * degrees, fa), BF16),
            vmem((mb, 2, degrees, 2 * chans), BF16),
            vmem((mb, 2, degrees, fa), F32),
            vmem((2 * chans, fa), BF16),
            vmem((4 * fields, 2 * chans), BF16),
            vmem((members, fa, nlon), BF16),
            vmem((bands, wide, fa), F32),
            vmem((bands, wide, fa), BF16),
            vmem((members * bands, wide, fa), BF16),
            vmem((fa, nlon), F32),
            vmem((pl.cdiv(nlon, LANES), fa, LANES), F32),
            vmem((fa, nlon), F32),
            dma((8,)),
            dma((4,)),
            dma((7,)),
            dma((pairs,)),
            dma((1,)),
            dma((members,)),
            plain((max(1, (bands - 1).bit_length()),)),
            plain((max(1, (members - 1).bit_length()),)),
        ],
        compiler_params=pltpu.CompilerParams(
            collective_id=0, has_side_effects=True, vmem_limit_bytes=60 * 1024 * 1024
        ),
    )(
        state,
        conv_weight,
        legendre,
        quad_weight.reshape(1, nlat),
        spectral_gain,
        project_weight.T,
        target,
        table,
    )
    return out.reshape(1, fields, lat_rows, nlon)


def solution(mesh):
    return jax.shard_map(
        local,
        mesh=mesh,
        in_specs=(
            P("member", "lat", None, None),
            P(),
            P("lat", None, None),
            P(),
            P(),
            P(),
            P(None, "lat", None),
        ),
        out_specs=P("member", None, "lat", None),
        check_vma=False,
    )
```

```python
import functools
import jax
import jax.numpy as jnp
import numpy as np
from jax import lax
from jax.experimental import pallas as pl
from jax.experimental.pallas import tpu as pltpu
from jax.sharding import PartitionSpec as P

MESH = pl.DeviceIdType.MESH
HALF = 4
LANES = 128
F32 = jnp.float32
BF16 = jnp.bfloat16


def dft_table(nlon, modes, bands):
    phase = np.arange(nlon)[:, None] * np.arange(modes)[None, :] % nlon
    angle = phase * (2.0 * np.pi / nlon)
    table = np.stack([np.cos(angle), -np.sin(angle)], axis=1) / np.sqrt(nlon)
    table = table.reshape(nlon, 2, bands, modes // bands).swapaxes(1, 2)
    return jnp.asarray(table.reshape(nlon, 2 * modes).T.astype(np.float32), BF16)


def dot(a, b, contract=((1,), (0,))):
    return lax.dot_general(a, b, (contract, ((), ())), preferred_element_type=F32)


def smooth(diff):
    return diff * lax.rsqrt(diff * diff + 0.25)


def kernel(
    members,
    bands,
    state,
    conv_hbm,
    leg_hbm,
    quad_hbm,
    gain_hbm,
    proj_hbm,
    target_hbm,
    table_hbm,
    out,
    rows,
    conv_w,
    leg,
    quad,
    gain,
    proj,
    target,
    table,
    toeplitz,
    mixed,
    spec,
    banded,
    spread,
    wtable,
    leg_t,
    gather,
    masked,
    filt,
    filtw,
    wrep,
    drep,
    directs,
    narrow,
    everyone,
    observed,
    own_rows,
    mine,
    load_sems,
    halo_sems,
    send_sems,
    spec_sems,
    direct_sems,
    back_sems,
    lat_sems,
    member_sems,
    left_sem,
):
    member, band = lax.axis_index("member"), lax.axis_index("lat")
    _, lat_rows, nlon, chans = state.shape
    pairs = lat_rows // 2
    nlat = bands * lat_rows
    mb, degrees = leg.shape[0], leg.shape[1]
    wide = 2 * mb
    fields = proj.shape[0]
    fa = fields * lat_rows
    lanes = [slice(i, min(i + LANES, nlon)) for i in range(0, nlon, LANES)]
    has_low, has_high = band > 0, band < bands - 1

    barrier = pltpu.get_barrier_semaphore()
    hops = [1 << i for i in range((members - 1).bit_length())]

    def greet_lat(sem, dist):
        @pl.when(band >= dist)
        def _():
            pl.semaphore_signal(sem, 1, device_id=(member, band - dist), device_id_type=MESH)

        @pl.when(band + dist < bands)
        def _():
            pl.semaphore_signal(sem, 1, device_id=(member, band + dist), device_id_type=MESH)

    def count_lat(dist):
        return (band >= dist).astype(jnp.int32) + (band + dist < bands).astype(jnp.int32)

    greet_lat(barrier, 1)
    for hop in hops:
        pl.semaphore_signal(barrier, 1, device_id=(member ^ hop, band), device_id_type=MESH)
    loads = [
        (state.at[0], rows.at[pl.ds(HALF, lat_rows)]),
        (conv_hbm, conv_w),
        (table_hbm, table),
        (leg_hbm, leg),
        (quad_hbm, quad),
        (gain_hbm, gain),
        (proj_hbm, proj),
        (target_hbm, target),
    ]
    loads = [pltpu.make_async_copy(a, b, load_sems.at[i]) for i, (a, b) in enumerate(loads)]
    for copy in loads:
        copy.start()
    pl.semaphore_wait(barrier, count_lat(1) + len(hops))

    rounds = []
    for i, hop in enumerate(hops[1:]):
        rounds.append((member_sems.at[i], hop, None))
    known = 1
    while known < bands - 1:
        rounds.append((lat_sems.at[len(rounds) - len(hops) + 1], None, known))
        known *= 2

    def round_signal(i):
        if i < len(rounds):
            sem, hop, dist = rounds[i]
            if hop is None:
                greet_lat(sem, dist)
            else:
                pl.semaphore_signal(sem, 1, device_id=(member ^ hop, band), device_id_type=MESH)

    def step_round(i):
        if i < len(rounds):
            sem, hop, dist = rounds[i]
            pl.semaphore_wait(sem, 1 if hop is not None else count_lat(dist))
            round_signal(i + 1)

    round_signal(0)

    def halo(up, far):
        if up:
            src = lat_rows - 2 - 2 * far
            dst = HALF - 2 - 2 * far
            peer = band + 1
        else:
            src = 2 * far
            dst = HALF + lat_rows + 2 * far
            peer = band - 1
        sem = 2 * (0 if up else 1) + far
        return pltpu.make_async_remote_copy(
            state.at[0, pl.ds(src, 2)],
            rows.at[pl.ds(dst, 2)],
            send_sems.at[sem],
            halo_sems.at[sem],
            device_id=(member, peer),
            device_id_type=MESH,
        )

    even = band % 2 == 0

    @pl.when(even & has_low)
    def _():
        halo(False, 0).start()
        halo(False, 1).start()

    @pl.when(has_high)
    def _():
        halo(True, 0).start()
        halo(True, 1).start()

    @pl.when(jnp.logical_not(even) & has_low)
    def _():
        halo(False, 0).start()
        halo(False, 1).start()

    @pl.when(jnp.logical_not(has_low))
    def _():
        rows[0:HALF] = jnp.zeros((HALF, nlon, chans), BF16)

    @pl.when(jnp.logical_not(has_high))
    def _():
        rows[HALF + lat_rows :] = jnp.zeros((HALF, nlon, chans), BF16)

    def halo_wait(low, far):
        @pl.when(has_low if low else has_high)
        def _():
            halo(low, far).wait_recv()

    loads[1].wait()
    taps = conv_w.shape[0]
    for d in range(HALF + 1):
        for e in (0, 1):
            for f in (0, 1):
                tap = 2 * d + e - f
                w = conv_w[tap] if 0 <= tap < taps else jnp.zeros((chans, chans), BF16)
                at = (2 * d + e) * chans
                toeplitz[at : at + chans, f * chans : (f + 1) * chans] = w
    def pair_of(t):
        return jnp.where(even, pairs - 1 - t, t)

    def convolve(t):
        p = pair_of(t)
        window = [rows[2 * p + j] for j in range(2 * HALF + 2)]
        conv = dot(jnp.concatenate(window, axis=1), toeplitz[...])
        own = jnp.concatenate([rows[2 * p + HALF], rows[2 * p + HALF + 1]], axis=1)
        half = conv * 0.5
        mixed[p] = (own.astype(F32) + half + half * jnp.tanh(half)).astype(BF16)

    def transform(t):
        p = pair_of(t)
        s = dot(table[...], mixed[p]).astype(BF16)
        for e in (0, 1):
            spec[:, p, e] = s[:, e * chans : (e + 1) * chans].reshape(bands, wide, chans)

    def send_spec(first, last):
        at = pl.ds(jnp.where(even, pairs - 1 - last, first), last - first + 1)
        arrival = spec_sems.at[first]

        def to(peer):
            pltpu.make_async_remote_copy(
                spec.at[peer, at], banded.at[band, at], send_sems.at[4], arrival,
                device_id=(member, peer), device_id_type=MESH,
            ).start()

        for dist in range(bands - 1, 0, -1):

            @pl.when(band + dist < bands)
            def _():
                to(band + dist)

            @pl.when(band >= dist)
            def _():
                to(band - dist)

        pltpu.make_async_copy(spec.at[band, at], banded.at[band, at], arrival).start()

    def wait_spec(first, last):
        part = banded.at[:, pl.ds(first, last - first + 1)]
        pltpu.make_async_copy(part, part, spec_sems.at[first]).wait()

    def direct(t):
        p = pair_of(t)
        fine = dot(drep[...], mixed[p], ((1,), (1,)))
        half = 2 * fields
        at = pl.ds(p * half, half)
        directs[member, at] = (fine[:half] + fine[half:]).astype(BF16)

        @pl.loop(1, members)
        def _(k):
            part = directs.at[member, at]
            pltpu.make_async_remote_copy(
                part, part, send_sems.at[5], direct_sems.at[0],
                device_id=(member ^ k, band), device_id_type=MESH,
            ).start()

    loads[6].wait()
    high = proj[...].astype(BF16)
    low = (proj[...] - high.astype(F32)).astype(BF16)
    r0 = lax.broadcasted_iota(jnp.int32, (fa, fields), 0) % fields
    r1 = lax.broadcasted_iota(jnp.int32, (fa, fields), 1)
    tile = jnp.where(r0 == r1, 1.0, 0.0).astype(BF16)
    tiled = dot(tile, high).T.astype(BF16)
    for r in (0, 1):
        wrep[r * chans : (r + 1) * chans, r * fa : (r + 1) * fa] = tiled
        wrep[r * chans : (r + 1) * chans, (1 - r) * fa : (2 - r) * fa] = jnp.zeros_like(tiled)
    for i, part in enumerate((high, low)):
        for e in (0, 1):
            at = (2 * i + e) * fields
            drep[at : at + fields, e * chans : (e + 1) * chans] = part
            drep[at : at + fields, (1 - e) * chans : (2 - e) * chans] = jnp.zeros_like(part)
    step_round(0)

    loads[0].wait()

    @pl.when(even)
    def _():
        halo_wait(False, 0)
        halo_wait(False, 1)

    @pl.when(jnp.logical_not(even))
    def _():
        halo_wait(True, 0)
        halo_wait(True, 1)

    convolve(0)
    step_round(1)
    loads[2].wait()
    transform(0)
    direct(0)
    convolve(1)
    step_round(2)
    transform(1)
    direct(1)

    @pl.when(even)
    def _():
        halo_wait(True, 0)

    @pl.when(jnp.logical_not(even))
    def _():
        halo_wait(False, 0)

    for t in range(2, pairs - 1):
        convolve(t)
        transform(t)
        direct(t)

    for i in (3, 4, 5, 7):
        loads[i].wait()
    wtable[...] = (leg[...].astype(F32) * quad[...]).astype(BF16)
    for m in range(mb):
        leg_t[m] = leg[m].T
    r0 = lax.broadcasted_iota(jnp.int32, (wide, wide * lat_rows), 0)
    r1 = lax.broadcasted_iota(jnp.int32, (wide, wide * lat_rows), 1)
    gather[...] = jnp.where(r1 // lat_rows == r0, 1.0, 0.0).astype(BF16)
    for i, at in enumerate(lanes):
        width = at.stop - at.start
        own_rows[i, :, :width] = target[:, :, at].astype(F32).reshape(fa, width)
        for a in range(lat_rows):
            rows_of = own_rows[i, pl.ds(a, fields, stride=lat_rows), :]
            observed[a * fields : (a + 1) * fields, at] = rows_of[:, :width]

    for i in range(3, len(rounds)):
        step_round(i)

    send_spec(0, 0)

    @pl.when(even & has_low)
    def _():
        halo(False, 0).wait_send()
        halo(False, 1).wait_send()

    @pl.when(jnp.logical_not(even) & has_high)
    def _():
        halo(True, 0).wait_send()
        halo(True, 1).wait_send()

    neighbour = band ^ 1
    leaves = jnp.where(even, has_low, has_high)
    near_leaves = jnp.where(even, neighbour < bands - 1, neighbour > 0)

    @pl.when(leaves & jnp.logical_not(near_leaves))
    def _():
        pl.semaphore_signal(left_sem.at[0], 1, device_id=(member, neighbour), device_id_type=MESH)

    @pl.when(near_leaves & jnp.logical_not(leaves))
    def _():
        pl.semaphore_wait(left_sem.at[0], 1)

    send_spec(1, pairs - 2)

    @pl.when(even)
    def _():
        halo_wait(True, 1)

    @pl.when(jnp.logical_not(even))
    def _():
        halo_wait(False, 1)

    convolve(pairs - 1)
    transform(pairs - 1)
    send_spec(pairs - 1, pairs - 1)
    direct(pairs - 1)

    wait_spec(0, 0)
    wait_spec(1, pairs - 2)
    wait_spec(pairs - 1, pairs - 1)
    spread[...] = banded[...].astype(F32).reshape(nlat * wide, chans)
    gain_re, gain_im = gain[0], gain[1]
    for m in range(mb):
        re = spread[pl.ds(m, nlat, stride=wide), :]
        im = spread[pl.ds(mb + m, nlat, stride=wide), :]
        coef = dot(wtable[m], jnp.concatenate([re, im], axis=1).astype(BF16))
        c0, c1 = coef[:, :chans], coef[:, chans:]
        real, imag = c0 * gain_re - c1 * gain_im, c0 * gain_im + c1 * gain_re
        filt[m] = jnp.concatenate([real, imag], axis=1).astype(BF16)
    filtw[...] = (
        dot(filt[...].reshape(mb * degrees, 2 * chans), wrep[...])
        .astype(BF16)
        .reshape(mb, degrees, 2 * fa)
    )

    r0 = lax.broadcasted_iota(jnp.int32, (nlat, fa), 0) % lat_rows
    r1 = lax.broadcasted_iota(jnp.int32, (nlat, fa), 1) // fields
    for m in range(mb):
        synth = dot(leg_t[m], filtw[m])
        for r in (0, 1):
            kept = jnp.where(r0 == r1, synth[:, r * fa : (r + 1) * fa], 0.0).astype(BF16)
            masked[:, r * mb + m] = kept.reshape(bands, lat_rows, fa)
    for s in range(bands):
        narrow[s] = dot(gather[...], masked[s].reshape(wide * lat_rows, fa)).astype(BF16)

    me = member * bands + band

    def back(k, s):
        pltpu.make_async_remote_copy(
            narrow.at[s], everyone.at[me], send_sems.at[6], back_sems.at[member],
            device_id=(member ^ k, s), device_id_type=MESH,
        ).start()

    @pl.loop(1, bands)
    def _(i):
        dist = bands - i

        @pl.when(band + dist < bands)
        def _():
            for k in range(members):
                back(members - 1 - k, band + dist)

        @pl.when(band >= dist)
        def _():
            for k in range(members):
                back(members - 1 - k, band - dist)

    for k in range(1, members):
        back(k, band)
    pltpu.make_async_copy(narrow.at[band], everyone.at[me], back_sems.at[member]).start()

    def back_wait(j):
        arrived = everyone.at[pl.ds(j * bands, bands)]
        pltpu.make_async_copy(arrived, arrived, back_sems.at[j]).wait()

    def projected(j):
        k = everyone[pl.ds(j * bands, bands)].reshape(bands * wide, fa)
        synth = dot(k, table[...], ((0,), (0,)))
        return (directs[j].astype(F32) + synth).astype(BF16).astype(F32)

    back_wait(member)
    own = projected(member)
    observed[...] = smooth(own - observed[...])
    mine[...] = own
    sent = directs.at[pl.ds(0, members - 1)]
    pltpu.make_async_copy(sent, sent, direct_sems.at[0]).wait()

    @pl.loop(1, members)
    def _(k):
        j = member ^ k
        back_wait(j)
        observed[...] -= smooth(mine[...] - projected(j)) * (1.0 / (members - 1))

    for i, at in enumerate(lanes):
        width = at.stop - at.start
        own_rows[i, :, :width] = observed[:, at]
        for f in range(fields):
            rows_of = own_rows[i, pl.ds(f, lat_rows, stride=fields), :]
            out[f * lat_rows : (f + 1) * lat_rows, at] = rows_of[:, :width]

    @pl.when(even & has_high)
    def _():
        halo(True, 0).wait_send()
        halo(True, 1).wait_send()

    @pl.when(jnp.logical_not(even) & has_low)
    def _():
        halo(False, 0).wait_send()
        halo(False, 1).wait_send()

    sent = banded.at[pl.ds(0, bands - 1)]
    pltpu.make_async_copy(sent, sent, send_sems.at[4]).wait()
    sent = directs.at[pl.ds(0, members - 1)]
    pltpu.make_async_copy(sent, sent, send_sems.at[5]).wait()

    sent = everyone.at[pl.ds(0, members * bands - 1)]
    pltpu.make_async_copy(sent, sent, send_sems.at[6]).wait()


def local(state, conv_weight, legendre, quad_weight, spectral_gain, project_weight, target):
    _, lat_rows, nlon, chans = state.shape
    mb, degrees, nlat = legendre.shape
    members, bands = lax.axis_size("member"), lax.axis_size("lat")
    fields = project_weight.shape[1]
    fa, wide, pairs = fields * lat_rows, 2 * mb, lat_rows // 2
    table = dft_table(nlon, mb * bands, bands)
    vmem = pltpu.VMEM
    dma, plain = pltpu.SemaphoreType.DMA, pltpu.SemaphoreType.REGULAR
    out = pl.pallas_call(
        functools.partial(kernel, members, bands),
        out_shape=pltpu.VMEM((fa, nlon), F32),
        in_specs=[pl.BlockSpec(memory_space=pl.ANY)] * 8,
        out_specs=pl.BlockSpec(memory_space=pltpu.VMEM),
        scratch_shapes=[
            vmem((lat_rows + 2 * HALF, nlon, chans), BF16),
            vmem(conv_weight.shape, BF16),
            vmem(legendre.shape, BF16),
            vmem((1, nlat), F32),
            vmem(spectral_gain.shape, F32),
            vmem((fields, chans), F32),
            vmem(target.shape, BF16),
            vmem(table.shape, BF16),
            vmem(((2 * HALF + 2) * chans, 2 * chans), BF16),
            vmem((pairs, nlon, 2 * chans), BF16),
            vmem((bands, pairs, 2, wide, chans), BF16),
            vmem((bands, pairs, 2, wide, chans), BF16),
            vmem((nlat * wide, chans), F32),
            vmem(legendre.shape, BF16),
            vmem((mb, nlat, degrees), BF16),
            vmem((wide, wide * lat_rows), BF16),
            vmem((bands, wide, lat_rows, fa), BF16),
            vmem((mb, degrees, 2 * chans), BF16),
            vmem((mb, degrees, 2 * fa), BF16),
            vmem((2 * chans, 2 * fa), BF16),
            vmem((4 * fields, 2 * chans), BF16),
            vmem((members, fa, nlon), BF16),
            vmem((bands, wide, fa), BF16),
            vmem((members * bands, wide, fa), BF16),
            vmem((fa, nlon), F32),
            vmem((pl.cdiv(nlon, LANES), fa, LANES), F32),
            vmem((fa, nlon), F32),
            dma((8,)),
            dma((4,)),
            dma((7,)),
            dma((pairs,)),
            dma((1,)),
            dma((members,)),
            plain((max(1, (bands - 1).bit_length()),)),
            plain((max(1, (members - 1).bit_length()),)),
            plain((1,)),
        ],
        compiler_params=pltpu.CompilerParams(
            collective_id=0, has_side_effects=True, vmem_limit_bytes=60 * 1024 * 1024
        ),
    )(
        state,
        conv_weight,
        legendre,
        quad_weight.reshape(1, nlat),
        spectral_gain,
        project_weight.T,
        target,
        table,
    )
    return out.reshape(1, fields, lat_rows, nlon)


def solution(mesh):
    return jax.shard_map(
        local,
        mesh=mesh,
        in_specs=(
            P("member", "lat", None, None),
            P(),
            P("lat", None, None),
            P(),
            P(),
            P(),
            P(None, "lat", None),
        ),
        out_specs=P("member", None, "lat", None),
        check_vma=False,
    )
```

```python
import functools
import jax
import jax.numpy as jnp
import numpy as np
from jax import lax
from jax.experimental import pallas as pl
from jax.experimental.pallas import tpu as pltpu
from jax.sharding import PartitionSpec as P

MESH = pl.DeviceIdType.MESH
HALF = 4
LANES = 128
VMEM_BYTES = 67043328
F32 = jnp.float32
BF16 = jnp.bfloat16


def dft_table(nlon, modes, bands):
    phase = np.arange(nlon)[:, None] * np.arange(modes)[None, :] % nlon
    angle = phase * (2.0 * np.pi / nlon)
    table = np.stack([np.cos(angle), -np.sin(angle)], axis=1) / np.sqrt(nlon)
    table = table.reshape(nlon, 2, bands, modes // bands).swapaxes(1, 2)
    return jnp.asarray(table.reshape(nlon, 2 * modes).T.astype(np.float32), BF16)


def dot(a, b, contract=((1,), (0,))):
    return lax.dot_general(a, b, (contract, ((), ())), preferred_element_type=F32)


def smooth(diff):
    return diff * lax.rsqrt(diff * diff + 0.25)


def kernel(
    members,
    bands,
    state,
    conv_hbm,
    leg_hbm,
    quad_hbm,
    gain_hbm,
    proj_hbm,
    target_hbm,
    table_hbm,
    everyone,
    directs,
    table,
    mine,
    observed,
    rows,
    conv_w,
    leg,
    quad,
    gain,
    proj,
    target,
    toeplitz,
    mixed,
    spec,
    banded,
    spread,
    wtable,
    leg_t,
    gather,
    masked,
    filt,
    filtw,
    wrep,
    drep,
    narrow,
    own_rows,
    load_sems,
    halo_sems,
    send_sems,
    spec_sems,
    direct_sems,
    back_sems,
    lat_sems,
    member_sems,
    left_sem,
):
    member, band = lax.axis_index("member"), lax.axis_index("lat")
    _, lat_rows, nlon, chans = state.shape
    pairs = lat_rows // 2
    nlat = bands * lat_rows
    mb, degrees = leg.shape[0], leg.shape[1]
    wide = 2 * mb
    fields = proj.shape[0]
    fa = fields * lat_rows
    lanes = [slice(i, min(i + LANES, nlon)) for i in range(0, nlon, LANES)]
    has_low, has_high = band > 0, band < bands - 1

    barrier = pltpu.get_barrier_semaphore()
    hops = [1 << i for i in range((members - 1).bit_length())]

    def greet_lat(sem, dist):
        @pl.when(band >= dist)
        def _():
            pl.semaphore_signal(sem, 1, device_id=(member, band - dist), device_id_type=MESH)

        @pl.when(band + dist < bands)
        def _():
            pl.semaphore_signal(sem, 1, device_id=(member, band + dist), device_id_type=MESH)

    def count_lat(dist):
        return (band >= dist).astype(jnp.int32) + (band + dist < bands).astype(jnp.int32)

    greet_lat(barrier, 1)
    for hop in hops:
        pl.semaphore_signal(barrier, 1, device_id=(member ^ hop, band), device_id_type=MESH)
    loads = [
        (state.at[0], rows.at[pl.ds(HALF, lat_rows)]),
        (conv_hbm, conv_w),
        (table_hbm, table),
        (leg_hbm, leg),
        (quad_hbm, quad),
        (gain_hbm, gain),
        (proj_hbm, proj),
        (target_hbm, target),
    ]
    loads = [pltpu.make_async_copy(a, b, load_sems.at[i]) for i, (a, b) in enumerate(loads)]
    for copy in loads:
        copy.start()
    pl.semaphore_wait(barrier, count_lat(1) + len(hops))

    rounds = []
    for i, hop in enumerate(hops[1:]):
        rounds.append((member_sems.at[i], hop, None))
    known = 1
    while known < bands - 1:
        rounds.append((lat_sems.at[len(rounds) - len(hops) + 1], None, known))
        known *= 2

    def round_signal(i):
        if i < len(rounds):
            sem, hop, dist = rounds[i]
            if hop is None:
                greet_lat(sem, dist)
            else:
                pl.semaphore_signal(sem, 1, device_id=(member ^ hop, band), device_id_type=MESH)

    def step_round(i):
        if i < len(rounds):
            sem, hop, dist = rounds[i]
            pl.semaphore_wait(sem, 1 if hop is not None else count_lat(dist))
            round_signal(i + 1)

    round_signal(0)

    def halo(up, far):
        if up:
            src = lat_rows - 2 - 2 * far
            dst = HALF - 2 - 2 * far
            peer = band + 1
        else:
            src = 2 * far
            dst = HALF + lat_rows + 2 * far
            peer = band - 1
        sem = 2 * (0 if up else 1) + far
        return pltpu.make_async_remote_copy(
            state.at[0, pl.ds(src, 2)],
            rows.at[pl.ds(dst, 2)],
            send_sems.at[sem],
            halo_sems.at[sem],
            device_id=(member, peer),
            device_id_type=MESH,
        )

    even = band % 2 == 0

    @pl.when(even & has_low)
    def _():
        halo(False, 0).start()
        halo(False, 1).start()

    @pl.when(has_high)
    def _():
        halo(True, 0).start()
        halo(True, 1).start()

    @pl.when(jnp.logical_not(even) & has_low)
    def _():
        halo(False, 0).start()
        halo(False, 1).start()

    @pl.when(jnp.logical_not(has_low))
    def _():
        rows[0:HALF] = jnp.zeros((HALF, nlon, chans), BF16)

    @pl.when(jnp.logical_not(has_high))
    def _():
        rows[HALF + lat_rows :] = jnp.zeros((HALF, nlon, chans), BF16)

    def halo_wait(low, far):
        @pl.when(has_low if low else has_high)
        def _():
            halo(low, far).wait_recv()

    loads[1].wait()
    taps = conv_w.shape[0]
    for d in range(HALF + 1):
        for e in (0, 1):
            for f in (0, 1):
                tap = 2 * d + e - f
                w = conv_w[tap] if 0 <= tap < taps else jnp.zeros((chans, chans), BF16)
                at = (2 * d + e) * chans
                toeplitz[at : at + chans, f * chans : (f + 1) * chans] = w
    def pair_of(t):
        return jnp.where(even, pairs - 1 - t, t)

    def convolve(t):
        p = pair_of(t)
        window = [rows[2 * p + j] for j in range(2 * HALF + 2)]
        conv = dot(jnp.concatenate(window, axis=1), toeplitz[...])
        own = jnp.concatenate([rows[2 * p + HALF], rows[2 * p + HALF + 1]], axis=1)
        half = conv * 0.5
        mixed[p] = (own.astype(F32) + half + half * jnp.tanh(half)).astype(BF16)

    def transform(t):
        p = pair_of(t)
        s = dot(table[...], mixed[p]).astype(BF16)
        for e in (0, 1):
            spec[:, p, e] = s[:, e * chans : (e + 1) * chans].reshape(bands, wide, chans)

    def send_spec(first, last):
        at = pl.ds(jnp.where(even, pairs - 1 - last, first), last - first + 1)
        arrival = spec_sems.at[first]

        def to(peer):
            pltpu.make_async_remote_copy(
                spec.at[peer, at], banded.at[band, at], send_sems.at[4], arrival,
                device_id=(member, peer), device_id_type=MESH,
            ).start()

        for dist in range(bands - 1, 0, -1):

            @pl.when(band >= dist)
            def _():
                to(band - dist)

        for dist in range(bands - 1, 0, -1):

            @pl.when(band + dist < bands)
            def _():
                to(band + dist)

        pltpu.make_async_copy(spec.at[band, at], banded.at[band, at], arrival).start()

    def wait_spec(first, last):
        part = banded.at[:, pl.ds(first, last - first + 1)]
        pltpu.make_async_copy(part, part, spec_sems.at[first]).wait()

    def direct(t):
        p = pair_of(t)
        fine = dot(drep[...], mixed[p], ((1,), (1,)))
        half = 2 * fields
        at = pl.ds(p * half, half)
        directs[member, at] = (fine[:half] + fine[half:]).astype(BF16)

        @pl.loop(1, members)
        def _(k):
            part = directs.at[member, at]
            pltpu.make_async_remote_copy(
                part, part, send_sems.at[5], direct_sems.at[0],
                device_id=(member ^ k, band), device_id_type=MESH,
            ).start()

    loads[6].wait()
    high = proj[...].astype(BF16)
    low = (proj[...] - high.astype(F32)).astype(BF16)
    r0 = lax.broadcasted_iota(jnp.int32, (fa, fields), 0) % fields
    r1 = lax.broadcasted_iota(jnp.int32, (fa, fields), 1)
    tile = jnp.where(r0 == r1, 1.0, 0.0).astype(BF16)
    tiled = dot(tile, high).T.astype(BF16)
    for r in (0, 1):
        wrep[r * chans : (r + 1) * chans, r * fa : (r + 1) * fa] = tiled
        wrep[r * chans : (r + 1) * chans, (1 - r) * fa : (2 - r) * fa] = jnp.zeros_like(tiled)
    for i, part in enumerate((high, low)):
        for e in (0, 1):
            at = (2 * i + e) * fields
            drep[at : at + fields, e * chans : (e + 1) * chans] = part
            drep[at : at + fields, (1 - e) * chans : (2 - e) * chans] = jnp.zeros_like(part)
    step_round(0)

    loads[0].wait()

    @pl.when(even)
    def _():
        halo_wait(False, 0)
        halo_wait(False, 1)

    @pl.when(jnp.logical_not(even))
    def _():
        halo_wait(True, 0)
        halo_wait(True, 1)

    convolve(0)
    step_round(1)
    loads[2].wait()
    transform(0)
    direct(0)
    convolve(1)
    step_round(2)
    transform(1)
    direct(1)

    @pl.when(even)
    def _():
        halo_wait(True, 0)

    @pl.when(jnp.logical_not(even))
    def _():
        halo_wait(False, 0)

    for t in range(2, pairs - 1):
        convolve(t)
        transform(t)
        direct(t)

    for i in (3, 4, 5, 7):
        loads[i].wait()
    wtable[...] = (leg[...].astype(F32) * quad[...]).astype(BF16)
    for m in range(mb):
        leg_t[m] = leg[m].T
    r0 = lax.broadcasted_iota(jnp.int32, (wide, wide * lat_rows), 0)
    r1 = lax.broadcasted_iota(jnp.int32, (wide, wide * lat_rows), 1)
    gather[...] = jnp.where(r1 // lat_rows == r0, 1.0, 0.0).astype(BF16)
    for i, at in enumerate(lanes):
        width = at.stop - at.start
        own_rows[i, :, :width] = target[:, :, at].astype(F32).reshape(fa, width)
        for a in range(lat_rows):
            rows_of = own_rows[i, pl.ds(a, fields, stride=lat_rows), :]
            observed[a * fields : (a + 1) * fields, at] = rows_of[:, :width]

    for i in range(3, len(rounds)):
        step_round(i)

    send_spec(0, 0)

    @pl.when(even & has_low)
    def _():
        halo(False, 0).wait_send()
        halo(False, 1).wait_send()

    @pl.when(jnp.logical_not(even) & has_high)
    def _():
        halo(True, 0).wait_send()
        halo(True, 1).wait_send()

    neighbour = band ^ 1
    leaves = jnp.where(even, has_low, has_high)
    near_leaves = jnp.where(even, neighbour < bands - 1, neighbour > 0)

    @pl.when(leaves & jnp.logical_not(near_leaves))
    def _():
        pl.semaphore_signal(left_sem.at[0], 1, device_id=(member, neighbour), device_id_type=MESH)

    @pl.when(near_leaves & jnp.logical_not(leaves))
    def _():
        pl.semaphore_wait(left_sem.at[0], 1)

    send_spec(1, pairs - 2)

    @pl.when(even)
    def _():
        halo_wait(True, 1)

    @pl.when(jnp.logical_not(even))
    def _():
        halo_wait(False, 1)

    convolve(pairs - 1)
    transform(pairs - 1)
    send_spec(pairs - 1, pairs - 1)
    direct(pairs - 1)

    def spread_rows(t):
        for source in range(bands):
            q = pairs - 1 - t if source % 2 == 0 else t
            at = (source * pairs + q) * 2 * wide
            spread[at : at + 2 * wide, :] = banded[source, q].astype(F32).reshape(2 * wide, chans)

    wait_spec(0, 0)
    wait_spec(1, pairs - 2)
    for t in range(pairs - 1):
        spread_rows(t)
    wait_spec(pairs - 1, pairs - 1)
    spread_rows(pairs - 1)
    gain_re, gain_im = gain[0], gain[1]
    for m in range(mb):
        re = spread[pl.ds(m, nlat, stride=wide), :]
        im = spread[pl.ds(mb + m, nlat, stride=wide), :]
        coef = dot(wtable[m], jnp.concatenate([re, im], axis=1).astype(BF16))
        c0, c1 = coef[:, :chans], coef[:, chans:]
        real, imag = c0 * gain_re - c1 * gain_im, c0 * gain_im + c1 * gain_re
        filt[m] = jnp.concatenate([real, imag], axis=1).astype(BF16)
    filtw[...] = (
        dot(filt[...].reshape(mb * degrees, 2 * chans), wrep[...])
        .astype(BF16)
        .reshape(mb, degrees, 2 * fa)
    )

    r0 = lax.broadcasted_iota(jnp.int32, (nlat, fa), 0) % lat_rows
    r1 = lax.broadcasted_iota(jnp.int32, (nlat, fa), 1) // fields
    for m in range(mb):
        synth = dot(leg_t[m], filtw[m])
        for r in (0, 1):
            kept = jnp.where(r0 == r1, synth[:, r * fa : (r + 1) * fa], 0.0).astype(BF16)
            masked[:, r * mb + m] = kept.reshape(bands, lat_rows, fa)
    for s in range(bands):
        narrow[s] = dot(gather[...], masked[s].reshape(wide * lat_rows, fa)).astype(BF16)

    me = member * bands + band

    def back(k, s):
        pltpu.make_async_remote_copy(
            narrow.at[s], everyone.at[me], send_sems.at[6], back_sems.at[member],
            device_id=(member ^ k, s), device_id_type=MESH,
        ).start()

    @pl.loop(1, bands)
    def _(i):
        dist = bands - i

        @pl.when(band >= dist)
        def _():
            for k in range(members):
                back(members - 1 - k, band - dist)

    @pl.loop(1, bands)
    def _(i):
        dist = bands - i

        @pl.when(band + dist < bands)
        def _():
            for k in range(members):
                back(members - 1 - k, band + dist)

    for k in range(1, members):
        back(k, band)
    pltpu.make_async_copy(narrow.at[band], everyone.at[me], back_sems.at[member]).start()

    def back_wait(j):
        arrived = everyone.at[pl.ds(j * bands, bands)]
        pltpu.make_async_copy(arrived, arrived, back_sems.at[j]).wait()

    def projected(j):
        k = everyone[pl.ds(j * bands, bands)].reshape(bands * wide, fa)
        synth = dot(k, table[...], ((0,), (0,)))
        return (directs[j].astype(F32) + synth).astype(BF16).astype(F32)

    back_wait(member)
    own = projected(member)
    observed[...] = smooth(own - observed[...])
    mine[...] = own
    sent = directs.at[pl.ds(0, members - 1)]
    pltpu.make_async_copy(sent, sent, direct_sems.at[0]).wait()

    @pl.loop(1, members - 1)
    def _(k):
        j = member ^ k
        back_wait(j)
        observed[...] -= smooth(mine[...] - projected(j)) * (1.0 / (members - 1))

    back_wait(member ^ (members - 1))

    @pl.when(even & has_high)
    def _():
        halo(True, 0).wait_send()
        halo(True, 1).wait_send()

    @pl.when(jnp.logical_not(even) & has_low)
    def _():
        halo(False, 0).wait_send()
        halo(False, 1).wait_send()

    sent = banded.at[pl.ds(0, bands - 1)]
    pltpu.make_async_copy(sent, sent, send_sems.at[4]).wait()
    sent = directs.at[pl.ds(0, members - 1)]
    pltpu.make_async_copy(sent, sent, send_sems.at[5]).wait()

    sent = everyone.at[pl.ds(0, members * bands - 1)]
    pltpu.make_async_copy(sent, sent, send_sems.at[6]).wait()


def finish_kernel(
    members, bands, everyone, directs, table, mine, grads, out, tiles, sorted_rows, sems
):
    fields, lat_rows, nlon = out.shape
    last = lax.axis_index("member") ^ (members - 1)
    fa = fields * lat_rows
    k = everyone[pl.ds(last * bands, bands)].reshape(-1, fa).T
    copies = []
    for i, start in enumerate(range(0, nlon, LANES)):
        width = min(LANES, nlon - start)
        at = slice(start, start + width)
        other = (directs[last, :, at].astype(F32) + dot(k, table[:, at])).astype(BF16)
        term = smooth(mine[:, at] - other.astype(F32)) * (1.0 / (members - 1))
        tiles[i, :, :width] = grads[:, at] - term
        for f in range(fields):
            rows_of = tiles[i, pl.ds(f, lat_rows, stride=fields), :]
            sorted_rows[f, :, at] = rows_of[:, :width]
        part = pl.ds(start, width)
        copies.append(
            pltpu.make_async_copy(sorted_rows.at[:, :, part], out.at[:, :, part], sems.at[i])
        )
        copies[-1].start()
    for copy in copies:
        copy.wait()


def local(state, conv_weight, legendre, quad_weight, spectral_gain, project_weight, target):
    _, lat_rows, nlon, chans = state.shape
    mb, degrees, nlat = legendre.shape
    members, bands = lax.axis_size("member"), lax.axis_size("lat")
    fields = project_weight.shape[1]
    fa, wide, pairs = fields * lat_rows, 2 * mb, lat_rows // 2
    table = dft_table(nlon, mb * bands, bands)
    vmem = pltpu.VMEM
    dma, plain = pltpu.SemaphoreType.DMA, pltpu.SemaphoreType.REGULAR
    results = [
        vmem((members * bands, wide, fa), BF16),
        vmem((members, fa, nlon), BF16),
        vmem(table.shape, BF16),
        vmem((fa, nlon), F32),
        vmem((fa, nlon), F32),
    ]
    kept = sum(
        int(np.prod(r.shape[:-1])) * pl.cdiv(r.shape[-1], LANES) * LANES * jnp.dtype(r.dtype).itemsize
        for r in results
    )
    arrived = pl.pallas_call(
        functools.partial(kernel, members, bands),
        out_shape=results,
        in_specs=[pl.BlockSpec(memory_space=pl.ANY)] * 8,
        out_specs=[pl.BlockSpec(memory_space=pltpu.VMEM)] * 5,
        scratch_shapes=[
            vmem((lat_rows + 2 * HALF, nlon, chans), BF16),
            vmem(conv_weight.shape, BF16),
            vmem(legendre.shape, BF16),
            vmem((1, nlat), F32),
            vmem(spectral_gain.shape, F32),
            vmem((fields, chans), F32),
            vmem(target.shape, BF16),
            vmem(((2 * HALF + 2) * chans, 2 * chans), BF16),
            vmem((pairs, nlon, 2 * chans), BF16),
            vmem((bands, pairs, 2, wide, chans), BF16),
            vmem((bands, pairs, 2, wide, chans), BF16),
            vmem((nlat * wide, chans), F32),
            vmem(legendre.shape, BF16),
            vmem((mb, nlat, degrees), BF16),
            vmem((wide, wide * lat_rows), BF16),
            vmem((bands, wide, lat_rows, fa), BF16),
            vmem((mb, degrees, 2 * chans), BF16),
            vmem((mb, degrees, 2 * fa), BF16),
            vmem((2 * chans, 2 * fa), BF16),
            vmem((4 * fields, 2 * chans), BF16),
            vmem((bands, wide, fa), BF16),
            vmem((pl.cdiv(nlon, LANES), fa, LANES), F32),
            dma((8,)),
            dma((4,)),
            dma((7,)),
            dma((pairs,)),
            dma((1,)),
            dma((members,)),
            plain((max(1, (bands - 1).bit_length()),)),
            plain((max(1, (members - 1).bit_length()),)),
            plain((1,)),
        ],
        compiler_params=pltpu.CompilerParams(
            collective_id=0,
            has_side_effects=True,
            vmem_limit_bytes=VMEM_BYTES - kept - 2 * 1024 * 1024,
        ),
    )(
        state,
        conv_weight,
        legendre,
        quad_weight.reshape(1, nlat),
        spectral_gain,
        project_weight.T,
        target,
        table,
    )
    tiles = pl.cdiv(nlon, LANES)
    out = pl.pallas_call(
        functools.partial(finish_kernel, members, bands),
        out_shape=jax.ShapeDtypeStruct((fields, lat_rows, nlon), F32),
        in_specs=[pl.BlockSpec(memory_space=pltpu.VMEM)] * 5,
        out_specs=pl.BlockSpec(memory_space=pl.ANY),
        scratch_shapes=[
            vmem((tiles, fa, LANES), F32),
            vmem((fields, lat_rows, nlon), F32),
            dma((tiles,)),
        ],
        compiler_params=pltpu.CompilerParams(vmem_limit_bytes=16 * 1024 * 1024),
    )(*arrived)
    return out[None]


def solution(mesh):
    return jax.shard_map(
        local,
        mesh=mesh,
        in_specs=(
            P("member", "lat", None, None),
            P(),
            P("lat", None, None),
            P(),
            P(),
            P(),
            P(None, "lat", None),
        ),
        out_specs=P("member", None, "lat", None),
        check_vma=False,
    )
```

```python
import functools
import jax
import jax.numpy as jnp
import numpy as np
from jax import lax
from jax.experimental import pallas as pl
from jax.experimental.pallas import tpu as pltpu
from jax.sharding import PartitionSpec as P

MESH = pl.DeviceIdType.MESH
HALF = 4
LANES = 128
VMEM_BYTES = 67043328
F32 = jnp.float32
BF16 = jnp.bfloat16


def dft_table(nlon, modes, bands):
    phase = np.arange(nlon)[:, None] * np.arange(modes)[None, :] % nlon
    angle = phase * (2.0 * np.pi / nlon)
    table = np.stack([np.cos(angle), -np.sin(angle)], axis=1) / np.sqrt(nlon)
    table = table.reshape(nlon, 2, bands, modes // bands).swapaxes(1, 2)
    return jnp.asarray(table.reshape(nlon, 2 * modes).T.astype(np.float32), BF16)


def dot(a, b, contract=((1,), (0,))):
    return lax.dot_general(a, b, (contract, ((), ())), preferred_element_type=F32)


def smooth(diff):
    return diff * lax.rsqrt(diff * diff + 0.25)


def kernel(
    members,
    bands,
    state,
    conv_hbm,
    leg_hbm,
    quad_hbm,
    gain_hbm,
    proj_hbm,
    target_hbm,
    table_hbm,
    everyone,
    directs,
    table,
    mine,
    observed,
    rows,
    conv_w,
    leg,
    quad,
    gain,
    proj,
    target,
    toeplitz,
    partial,
    mixed,
    spec,
    banded,
    spread,
    wtable,
    leg_t,
    gather,
    masked,
    filt,
    filtw,
    wrep,
    drep,
    narrow,
    own_rows,
    load_sems,
    halo_sems,
    send_sems,
    spec_sems,
    direct_sems,
    back_sems,
    lat_sems,
    member_sems,
    left_sem,
):
    member, band = lax.axis_index("member"), lax.axis_index("lat")
    _, lat_rows, nlon, chans = state.shape
    pairs = lat_rows // 2
    nlat = bands * lat_rows
    mb, degrees = leg.shape[0], leg.shape[1]
    wide = 2 * mb
    fields = proj.shape[0]
    fa = fields * lat_rows
    lanes = [slice(i, min(i + LANES, nlon)) for i in range(0, nlon, LANES)]
    has_low, has_high = band > 0, band < bands - 1

    barrier = pltpu.get_barrier_semaphore()
    hops = [1 << i for i in range((members - 1).bit_length())]

    def greet_lat(sem, dist):
        @pl.when(band >= dist)
        def _():
            pl.semaphore_signal(sem, 1, device_id=(member, band - dist), device_id_type=MESH)

        @pl.when(band + dist < bands)
        def _():
            pl.semaphore_signal(sem, 1, device_id=(member, band + dist), device_id_type=MESH)

    def count_lat(dist):
        return (band >= dist).astype(jnp.int32) + (band + dist < bands).astype(jnp.int32)

    greet_lat(barrier, 1)
    for hop in hops:
        pl.semaphore_signal(barrier, 1, device_id=(member ^ hop, band), device_id_type=MESH)
    loads = [
        (state.at[0], rows.at[pl.ds(HALF, lat_rows)]),
        (conv_hbm, conv_w),
        (table_hbm, table),
        (leg_hbm, leg),
        (quad_hbm, quad),
        (gain_hbm, gain),
        (proj_hbm, proj),
        (target_hbm, target),
    ]
    loads = [pltpu.make_async_copy(a, b, load_sems.at[i]) for i, (a, b) in enumerate(loads)]
    for copy in loads:
        copy.start()
    pl.semaphore_wait(barrier, count_lat(1) + len(hops))

    rounds = []
    for i, hop in enumerate(hops[1:]):
        rounds.append((member_sems.at[i], hop, None))
    known = 1
    while known < bands - 1:
        rounds.append((lat_sems.at[len(rounds) - len(hops) + 1], None, known))
        known *= 2

    def round_signal(i):
        if i < len(rounds):
            sem, hop, dist = rounds[i]
            if hop is None:
                greet_lat(sem, dist)
            else:
                pl.semaphore_signal(sem, 1, device_id=(member ^ hop, band), device_id_type=MESH)

    def step_round(i):
        if i < len(rounds):
            sem, hop, dist = rounds[i]
            pl.semaphore_wait(sem, 1 if hop is not None else count_lat(dist))
            round_signal(i + 1)

    round_signal(0)

    def halo(up, far):
        if up:
            src = lat_rows - 2 - 2 * far
            dst = HALF - 2 - 2 * far
            peer = band + 1
        else:
            src = 2 * far
            dst = HALF + lat_rows + 2 * far
            peer = band - 1
        sem = 2 * (0 if up else 1) + far
        return pltpu.make_async_remote_copy(
            state.at[0, pl.ds(src, 2)],
            rows.at[pl.ds(dst, 2)],
            send_sems.at[sem],
            halo_sems.at[sem],
            device_id=(member, peer),
            device_id_type=MESH,
        )

    even = band % 2 == 0

    @pl.when(even & has_low)
    def _():
        halo(False, 0).start()
        halo(False, 1).start()

    @pl.when(has_high)
    def _():
        halo(True, 0).start()
        halo(True, 1).start()

    @pl.when(jnp.logical_not(even) & has_low)
    def _():
        halo(False, 0).start()
        halo(False, 1).start()

    @pl.when(jnp.logical_not(has_low))
    def _():
        rows[0:HALF] = jnp.zeros((HALF, nlon, chans), BF16)

    @pl.when(jnp.logical_not(has_high))
    def _():
        rows[HALF + lat_rows :] = jnp.zeros((HALF, nlon, chans), BF16)

    def halo_wait(low, far):
        @pl.when(has_low if low else has_high)
        def _():
            halo(low, far).wait_recv()

    loads[1].wait()
    taps = conv_w.shape[0]
    for d in range(HALF + 1):
        for e in (0, 1):
            for f in (0, 1):
                tap = 2 * d + e - f
                w = conv_w[tap] if 0 <= tap < taps else jnp.zeros((chans, chans), BF16)
                at = (2 * d + e) * chans
                toeplitz[at : at + chans, f * chans : (f + 1) * chans] = w
    def pair_of(t):
        return jnp.where(even, pairs - 1 - t, t)

    def mix(p, conv):
        own = jnp.concatenate([rows[2 * p + HALF], rows[2 * p + HALF + 1]], axis=1)
        half = conv * 0.5
        mixed[p] = (own.astype(F32) + half + half * jnp.tanh(half)).astype(BF16)

    def window_sum(p, first, count):
        window = [rows[2 * (p + first) + j] for j in range(2 * count)]
        at = pl.ds(pl.multiple_of(first * 2 * chans, 2 * chans), count * 2 * chans)
        return dot(jnp.concatenate(window, axis=1), toeplitz[at, :])

    def convolve(t):
        p = pair_of(t)
        mix(p, window_sum(p, 0, HALF + 1))

    def transform(t):
        p = pair_of(t)
        s = dot(table[...], mixed[p]).astype(BF16)
        for e in (0, 1):
            spec[:, p, e] = s[:, e * chans : (e + 1) * chans].reshape(bands, wide, chans)

    def send_spec(first, last):
        at = pl.ds(jnp.where(even, pairs - 1 - last, first), last - first + 1)
        arrival = spec_sems.at[first]

        def to(peer):
            pltpu.make_async_remote_copy(
                spec.at[peer, at], banded.at[band, at], send_sems.at[4], arrival,
                device_id=(member, peer), device_id_type=MESH,
            ).start()

        for dist in range(bands - 1, 0, -1):

            @pl.when(band >= dist)
            def _():
                to(band - dist)

        for dist in range(bands - 1, 0, -1):

            @pl.when(band + dist < bands)
            def _():
                to(band + dist)

        pltpu.make_async_copy(spec.at[band, at], banded.at[band, at], arrival).start()

    def wait_spec(first, last):
        part = banded.at[:, pl.ds(first, last - first + 1)]
        pltpu.make_async_copy(part, part, spec_sems.at[first]).wait()

    def direct(t):
        p = pair_of(t)
        fine = dot(drep[...], mixed[p], ((1,), (1,)))
        half = 2 * fields
        at = pl.ds(p * half, half)
        directs[member, at] = (fine[:half] + fine[half:]).astype(BF16)

        @pl.loop(1, members)
        def _(k):
            part = directs.at[member, at]
            pltpu.make_async_remote_copy(
                part, part, send_sems.at[5], direct_sems.at[0],
                device_id=(member ^ k, band), device_id_type=MESH,
            ).start()

    loads[6].wait()
    high = proj[...].astype(BF16)
    low = (proj[...] - high.astype(F32)).astype(BF16)
    r0 = lax.broadcasted_iota(jnp.int32, (fa, fields), 0) % fields
    r1 = lax.broadcasted_iota(jnp.int32, (fa, fields), 1)
    tile = jnp.where(r0 == r1, 1.0, 0.0).astype(BF16)
    tiled = dot(tile, high).T.astype(BF16)
    for r in (0, 1):
        wrep[r * chans : (r + 1) * chans, r * fa : (r + 1) * fa] = tiled
        wrep[r * chans : (r + 1) * chans, (1 - r) * fa : (2 - r) * fa] = jnp.zeros_like(tiled)
    for i, part in enumerate((high, low)):
        for e in (0, 1):
            at = (2 * i + e) * fields
            drep[at : at + fields, e * chans : (e + 1) * chans] = part
            drep[at : at + fields, (1 - e) * chans : (2 - e) * chans] = jnp.zeros_like(part)
    step_round(0)

    loads[0].wait()

    @pl.when(even)
    def _():
        halo_wait(False, 0)
        halo_wait(False, 1)

    @pl.when(jnp.logical_not(even))
    def _():
        halo_wait(True, 0)
        halo_wait(True, 1)

    convolve(0)
    step_round(1)
    loads[2].wait()
    transform(0)
    direct(0)
    convolve(1)
    step_round(2)
    transform(1)
    direct(1)

    @pl.when(even)
    def _():
        halo_wait(True, 0)

    @pl.when(jnp.logical_not(even))
    def _():
        halo_wait(False, 0)

    for t in range(2, pairs - 1):
        convolve(t)
        transform(t)
        direct(t)

    for i in (3, 4, 5, 7):
        loads[i].wait()
    wtable[...] = (leg[...].astype(F32) * quad[...]).astype(BF16)
    for m in range(mb):
        leg_t[m] = leg[m].T
    r0 = lax.broadcasted_iota(jnp.int32, (wide, wide * lat_rows), 0)
    r1 = lax.broadcasted_iota(jnp.int32, (wide, wide * lat_rows), 1)
    gather[...] = jnp.where(r1 // lat_rows == r0, 1.0, 0.0).astype(BF16)
    for i, at in enumerate(lanes):
        width = at.stop - at.start
        own_rows[i, :, :width] = target[:, :, at].astype(F32).reshape(fa, width)
        for a in range(lat_rows):
            rows_of = own_rows[i, pl.ds(a, fields, stride=lat_rows), :]
            observed[a * fields : (a + 1) * fields, at] = rows_of[:, :width]

    for i in range(3, len(rounds)):
        step_round(i)

    send_spec(0, 0)

    @pl.when(even & has_low)
    def _():
        halo(False, 0).wait_send()
        halo(False, 1).wait_send()

    @pl.when(jnp.logical_not(even) & has_high)
    def _():
        halo(True, 0).wait_send()
        halo(True, 1).wait_send()

    neighbour = band ^ 1
    leaves = jnp.where(even, has_low, has_high)
    near_leaves = jnp.where(even, neighbour < bands - 1, neighbour > 0)

    @pl.when(leaves & jnp.logical_not(near_leaves))
    def _():
        pl.semaphore_signal(left_sem.at[0], 1, device_id=(member, neighbour), device_id_type=MESH)

    @pl.when(near_leaves & jnp.logical_not(leaves))
    def _():
        pl.semaphore_wait(left_sem.at[0], 1)

    send_spec(1, pairs - 2)

    final_pair = pair_of(pairs - 1)
    partial[...] = window_sum(final_pair, jnp.where(even, 1, 0), HALF)

    @pl.when(even)
    def _():
        halo_wait(True, 1)

    @pl.when(jnp.logical_not(even))
    def _():
        halo_wait(False, 1)

    mix(final_pair, partial[...] + window_sum(final_pair, jnp.where(even, 0, HALF), 1))
    transform(pairs - 1)
    send_spec(pairs - 1, pairs - 1)
    direct(pairs - 1)

    def spread_rows(t):
        for source in range(bands):
            q = pairs - 1 - t if source % 2 == 0 else t
            at = (source * pairs + q) * 2 * wide
            spread[at : at + 2 * wide, :] = banded[source, q].astype(F32).reshape(2 * wide, chans)

    wait_spec(0, 0)
    wait_spec(1, pairs - 2)
    for t in range(pairs - 1):
        spread_rows(t)
    wait_spec(pairs - 1, pairs - 1)
    spread_rows(pairs - 1)
    gain_re, gain_im = gain[0], gain[1]
    for m in range(mb):
        re = spread[pl.ds(m, nlat, stride=wide), :]
        im = spread[pl.ds(mb + m, nlat, stride=wide), :]
        coef = dot(wtable[m], jnp.concatenate([re, im], axis=1).astype(BF16))
        c0, c1 = coef[:, :chans], coef[:, chans:]
        real, imag = c0 * gain_re - c1 * gain_im, c0 * gain_im + c1 * gain_re
        filt[m] = jnp.concatenate([real, imag], axis=1).astype(BF16)
    filtw[...] = (
        dot(filt[...].reshape(mb * degrees, 2 * chans), wrep[...])
        .astype(BF16)
        .reshape(mb, degrees, 2 * fa)
    )

    r0 = lax.broadcasted_iota(jnp.int32, (nlat, fa), 0) % lat_rows
    r1 = lax.broadcasted_iota(jnp.int32, (nlat, fa), 1) // fields
    for m in range(mb):
        synth = dot(leg_t[m], filtw[m])
        for r in (0, 1):
            kept = jnp.where(r0 == r1, synth[:, r * fa : (r + 1) * fa], 0.0).astype(BF16)
            masked[:, r * mb + m] = kept.reshape(bands, lat_rows, fa)
    for s in range(bands):
        narrow[s] = dot(gather[...], masked[s].reshape(wide * lat_rows, fa)).astype(BF16)

    me = member * bands + band

    def back(k, s):
        pltpu.make_async_remote_copy(
            narrow.at[s], everyone.at[me], send_sems.at[6], back_sems.at[member],
            device_id=(member ^ k, s), device_id_type=MESH,
        ).start()

    for dest in range(members):

        @pl.loop(0, bands)
        def _(s):
            @pl.when((s != band) | (member != dest))
            def _():
                back(member ^ dest, s)

    pltpu.make_async_copy(narrow.at[band], everyone.at[me], back_sems.at[member]).start()

    def back_wait(j):
        arrived = everyone.at[pl.ds(j * bands, bands)]
        pltpu.make_async_copy(arrived, arrived, back_sems.at[j]).wait()

    def projected(j):
        k = everyone[pl.ds(j * bands, bands)].reshape(bands * wide, fa)
        synth = dot(k, table[...], ((0,), (0,)))
        return (directs[j].astype(F32) + synth).astype(BF16).astype(F32)

    back_wait(member)
    own = projected(member)
    observed[...] = smooth(own - observed[...])
    mine[...] = own
    sent = directs.at[pl.ds(0, members - 1)]
    pltpu.make_async_copy(sent, sent, direct_sems.at[0]).wait()

    @pl.loop(1, members - 1)
    def _(k):
        j = member ^ k
        back_wait(j)
        observed[...] -= smooth(mine[...] - projected(j)) * (1.0 / (members - 1))

    back_wait(member ^ (members - 1))

    @pl.when(even & has_high)
    def _():
        halo(True, 0).wait_send()
        halo(True, 1).wait_send()

    @pl.when(jnp.logical_not(even) & has_low)
    def _():
        halo(False, 0).wait_send()
        halo(False, 1).wait_send()

    sent = banded.at[pl.ds(0, bands - 1)]
    pltpu.make_async_copy(sent, sent, send_sems.at[4]).wait()
    sent = directs.at[pl.ds(0, members - 1)]
    pltpu.make_async_copy(sent, sent, send_sems.at[5]).wait()

    sent = everyone.at[pl.ds(0, members * bands - 1)]
    pltpu.make_async_copy(sent, sent, send_sems.at[6]).wait()


def finish_kernel(
    members, bands, everyone, directs, table, mine, grads, out, tiles, sorted_rows, sems
):
    fields, lat_rows, nlon = out.shape
    last = lax.axis_index("member") ^ (members - 1)
    fa = fields * lat_rows
    k = everyone[pl.ds(last * bands, bands)].reshape(-1, fa).T
    copies = []
    for i, start in enumerate(range(0, nlon, LANES)):
        width = min(LANES, nlon - start)
        at = slice(start, start + width)
        other = (directs[last, :, at].astype(F32) + dot(k, table[:, at])).astype(BF16)
        term = smooth(mine[:, at] - other.astype(F32)) * (1.0 / (members - 1))
        tiles[i, :, :width] = grads[:, at] - term
        for f in range(fields):
            rows_of = tiles[i, pl.ds(f, lat_rows, stride=fields), :]
            sorted_rows[f, :, at] = rows_of[:, :width]
        part = pl.ds(start, width)
        copies.append(
            pltpu.make_async_copy(sorted_rows.at[:, :, part], out.at[:, :, part], sems.at[i])
        )
        copies[-1].start()
    for copy in copies:
        copy.wait()


def local(state, conv_weight, legendre, quad_weight, spectral_gain, project_weight, target):
    _, lat_rows, nlon, chans = state.shape
    mb, degrees, nlat = legendre.shape
    members, bands = lax.axis_size("member"), lax.axis_size("lat")
    fields = project_weight.shape[1]
    fa, wide, pairs = fields * lat_rows, 2 * mb, lat_rows // 2
    table = dft_table(nlon, mb * bands, bands)
    vmem = pltpu.VMEM
    dma, plain = pltpu.SemaphoreType.DMA, pltpu.SemaphoreType.REGULAR
    results = [
        vmem((members * bands, wide, fa), BF16),
        vmem((members, fa, nlon), BF16),
        vmem(table.shape, BF16),
        vmem((fa, nlon), F32),
        vmem((fa, nlon), F32),
    ]
    kept = sum(
        int(np.prod(r.shape[:-1])) * pl.cdiv(r.shape[-1], LANES) * LANES * jnp.dtype(r.dtype).itemsize
        for r in results
    )
    arrived = pl.pallas_call(
        functools.partial(kernel, members, bands),
        out_shape=results,
        in_specs=[pl.BlockSpec(memory_space=pl.ANY)] * 8,
        out_specs=[pl.BlockSpec(memory_space=pltpu.VMEM)] * 5,
        scratch_shapes=[
            vmem((lat_rows + 2 * HALF, nlon, chans), BF16),
            vmem(conv_weight.shape, BF16),
            vmem(legendre.shape, BF16),
            vmem((1, nlat), F32),
            vmem(spectral_gain.shape, F32),
            vmem((fields, chans), F32),
            vmem(target.shape, BF16),
            vmem(((2 * HALF + 2) * chans, 2 * chans), BF16),
            vmem((nlon, 2 * chans), F32),
            vmem((pairs, nlon, 2 * chans), BF16),
            vmem((bands, pairs, 2, wide, chans), BF16),
            vmem((bands, pairs, 2, wide, chans), BF16),
            vmem((nlat * wide, chans), F32),
            vmem(legendre.shape, BF16),
            vmem((mb, nlat, degrees), BF16),
            vmem((wide, wide * lat_rows), BF16),
            vmem((bands, wide, lat_rows, fa), BF16),
            vmem((mb, degrees, 2 * chans), BF16),
            vmem((mb, degrees, 2 * fa), BF16),
            vmem((2 * chans, 2 * fa), BF16),
            vmem((4 * fields, 2 * chans), BF16),
            vmem((bands, wide, fa), BF16),
            vmem((pl.cdiv(nlon, LANES), fa, LANES), F32),
            dma((8,)),
            dma((4,)),
            dma((7,)),
            dma((pairs,)),
            dma((1,)),
            dma((members,)),
            plain((max(1, (bands - 1).bit_length()),)),
            plain((max(1, (members - 1).bit_length()),)),
            plain((1,)),
        ],
        compiler_params=pltpu.CompilerParams(
            collective_id=0,
            has_side_effects=True,
            vmem_limit_bytes=VMEM_BYTES - kept - 2 * 1024 * 1024,
        ),
    )(
        state,
        conv_weight,
        legendre,
        quad_weight.reshape(1, nlat),
        spectral_gain,
        project_weight.T,
        target,
        table,
    )
    tiles = pl.cdiv(nlon, LANES)
    out = pl.pallas_call(
        functools.partial(finish_kernel, members, bands),
        out_shape=jax.ShapeDtypeStruct((fields, lat_rows, nlon), F32),
        in_specs=[pl.BlockSpec(memory_space=pltpu.VMEM)] * 5,
        out_specs=pl.BlockSpec(memory_space=pl.ANY),
        scratch_shapes=[
            vmem((tiles, fa, LANES), F32),
            vmem((fields, lat_rows, nlon), F32),
            dma((tiles,)),
        ],
        compiler_params=pltpu.CompilerParams(vmem_limit_bytes=16 * 1024 * 1024),
    )(*arrived)
    return out[None]


def solution(mesh):
    return jax.shard_map(
        local,
        mesh=mesh,
        in_specs=(
            P("member", "lat", None, None),
            P(),
            P("lat", None, None),
            P(),
            P(),
            P(),
            P(None, "lat", None),
        ),
        out_specs=P("member", None, "lat", None),
        check_vma=False,
    )
```

```python
import functools
import jax
import jax.numpy as jnp
import numpy as np
from jax import lax
from jax.experimental import pallas as pl
from jax.experimental.pallas import tpu as pltpu
from jax.sharding import PartitionSpec as P

MESH = pl.DeviceIdType.MESH
HALF = 4
LANES = 128
VMEM_BYTES = 67043328
F32 = jnp.float32
BF16 = jnp.bfloat16


def dft_table(nlon, modes, bands):
    phase = np.arange(nlon)[:, None] * np.arange(modes)[None, :] % nlon
    angle = phase * (2.0 * np.pi / nlon)
    table = np.stack([np.cos(angle), -np.sin(angle)], axis=1) / np.sqrt(nlon)
    table = table.reshape(nlon, 2, bands, modes // bands).swapaxes(1, 2)
    return jnp.asarray(table.reshape(nlon, 2 * modes).T.astype(np.float32), BF16)


def dot(a, b, contract=((1,), (0,))):
    return lax.dot_general(a, b, (contract, ((), ())), preferred_element_type=F32)


def smooth(diff):
    return diff * lax.rsqrt(diff * diff + 0.25)


def kernel(
    members,
    bands,
    state,
    conv_hbm,
    leg_hbm,
    quad_hbm,
    gain_hbm,
    proj_hbm,
    target_hbm,
    table_hbm,
    everyone,
    directs,
    table,
    mine,
    observed,
    rows,
    conv_w,
    leg,
    quad,
    gain,
    proj,
    target,
    toeplitz,
    partial,
    mixed,
    spec,
    banded,
    spread,
    wearly,
    wlate,
    early,
    leg_t,
    gather,
    masked,
    filt,
    filtw,
    wrep,
    drep,
    narrow,
    own_rows,
    load_sems,
    halo_sems,
    send_sems,
    spec_sems,
    direct_sems,
    back_sems,
    lat_sems,
    member_sems,
    left_sem,
):
    member, band = lax.axis_index("member"), lax.axis_index("lat")
    _, lat_rows, nlon, chans = state.shape
    pairs = lat_rows // 2
    nlat = bands * lat_rows
    mb, degrees = leg.shape[0], leg.shape[1]
    wide = 2 * mb
    fields = proj.shape[0]
    fa = fields * lat_rows
    lanes = [slice(i, min(i + LANES, nlon)) for i in range(0, nlon, LANES)]
    has_low, has_high = band > 0, band < bands - 1

    barrier = pltpu.get_barrier_semaphore()
    hops = [1 << i for i in range((members - 1).bit_length())]

    def greet_lat(sem, dist):
        @pl.when(band >= dist)
        def _():
            pl.semaphore_signal(sem, 1, device_id=(member, band - dist), device_id_type=MESH)

        @pl.when(band + dist < bands)
        def _():
            pl.semaphore_signal(sem, 1, device_id=(member, band + dist), device_id_type=MESH)

    def count_lat(dist):
        return (band >= dist).astype(jnp.int32) + (band + dist < bands).astype(jnp.int32)

    greet_lat(barrier, 1)
    for hop in hops:
        pl.semaphore_signal(barrier, 1, device_id=(member ^ hop, band), device_id_type=MESH)
    loads = [
        (state.at[0], rows.at[pl.ds(HALF, lat_rows)]),
        (conv_hbm, conv_w),
        (table_hbm, table),
        (leg_hbm, leg),
        (quad_hbm, quad),
        (gain_hbm, gain),
        (proj_hbm, proj),
        (target_hbm, target),
    ]
    loads = [pltpu.make_async_copy(a, b, load_sems.at[i]) for i, (a, b) in enumerate(loads)]
    for copy in loads:
        copy.start()
    pl.semaphore_wait(barrier, count_lat(1) + len(hops))

    rounds = []
    for i, hop in enumerate(hops[1:]):
        rounds.append((member_sems.at[i], hop, None))
    known = 1
    while known < bands - 1:
        rounds.append((lat_sems.at[len(rounds) - len(hops) + 1], None, known))
        known *= 2

    def round_signal(i):
        if i < len(rounds):
            sem, hop, dist = rounds[i]
            if hop is None:
                greet_lat(sem, dist)
            else:
                pl.semaphore_signal(sem, 1, device_id=(member ^ hop, band), device_id_type=MESH)

    def step_round(i):
        if i < len(rounds):
            sem, hop, dist = rounds[i]
            pl.semaphore_wait(sem, 1 if hop is not None else count_lat(dist))
            round_signal(i + 1)

    round_signal(0)

    def halo(up, far):
        if up:
            src = lat_rows - 2 - 2 * far
            dst = HALF - 2 - 2 * far
            peer = band + 1
        else:
            src = 2 * far
            dst = HALF + lat_rows + 2 * far
            peer = band - 1
        sem = 2 * (0 if up else 1) + far
        return pltpu.make_async_remote_copy(
            state.at[0, pl.ds(src, 2)],
            rows.at[pl.ds(dst, 2)],
            send_sems.at[sem],
            halo_sems.at[sem],
            device_id=(member, peer),
            device_id_type=MESH,
        )

    even = band % 2 == 0

    @pl.when(even & has_low)
    def _():
        halo(False, 0).start()
        halo(False, 1).start()

    @pl.when(has_high)
    def _():
        halo(True, 0).start()
        halo(True, 1).start()

    @pl.when(jnp.logical_not(even) & has_low)
    def _():
        halo(False, 0).start()
        halo(False, 1).start()

    @pl.when(jnp.logical_not(has_low))
    def _():
        rows[0:HALF] = jnp.zeros((HALF, nlon, chans), BF16)

    @pl.when(jnp.logical_not(has_high))
    def _():
        rows[HALF + lat_rows :] = jnp.zeros((HALF, nlon, chans), BF16)

    def halo_wait(low, far):
        @pl.when(has_low if low else has_high)
        def _():
            halo(low, far).wait_recv()

    loads[1].wait()
    taps = conv_w.shape[0]
    for d in range(HALF + 1):
        for e in (0, 1):
            for f in (0, 1):
                tap = 2 * d + e - f
                w = conv_w[tap] if 0 <= tap < taps else jnp.zeros((chans, chans), BF16)
                at = (2 * d + e) * chans
                toeplitz[at : at + chans, f * chans : (f + 1) * chans] = w
    def pair_of(t):
        return jnp.where(even, pairs - 1 - t, t)

    def mix(p, conv):
        own = jnp.concatenate([rows[2 * p + HALF], rows[2 * p + HALF + 1]], axis=1)
        half = conv * 0.5
        mixed[p] = (own.astype(F32) + half + half * jnp.tanh(half)).astype(BF16)

    def window_sum(p, first, count):
        window = [rows[2 * (p + first) + j] for j in range(2 * count)]
        at = pl.ds(pl.multiple_of(first * 2 * chans, 2 * chans), count * 2 * chans)
        return dot(jnp.concatenate(window, axis=1), toeplitz[at, :])

    def convolve(t):
        p = pair_of(t)
        mix(p, window_sum(p, 0, HALF + 1))

    def transform(t):
        p = pair_of(t)
        s = dot(table[...], mixed[p]).astype(BF16)
        for e in (0, 1):
            spec[:, p, e] = s[:, e * chans : (e + 1) * chans].reshape(bands, wide, chans)

    def send_spec(first, last):
        at = pl.ds(jnp.where(even, pairs - 1 - last, first), last - first + 1)
        arrival = spec_sems.at[first]

        def to(peer):
            pltpu.make_async_remote_copy(
                spec.at[peer, at], banded.at[band, at], send_sems.at[4], arrival,
                device_id=(member, peer), device_id_type=MESH,
            ).start()

        for dist in range(bands - 1, 0, -1):

            @pl.when(band >= dist)
            def _():
                to(band - dist)

        for dist in range(bands - 1, 0, -1):

            @pl.when(band + dist < bands)
            def _():
                to(band + dist)

        pltpu.make_async_copy(spec.at[band, at], banded.at[band, at], arrival).start()

    def wait_spec(first, last):
        part = banded.at[:, pl.ds(first, last - first + 1)]
        pltpu.make_async_copy(part, part, spec_sems.at[first]).wait()

    def direct(t):
        p = pair_of(t)
        fine = dot(drep[...], mixed[p], ((1,), (1,)))
        half = 2 * fields
        at = pl.ds(p * half, half)
        directs[member, at] = (fine[:half] + fine[half:]).astype(BF16)

        @pl.loop(1, members)
        def _(k):
            part = directs.at[member, at]
            pltpu.make_async_remote_copy(
                part, part, send_sems.at[5], direct_sems.at[0],
                device_id=(member ^ k, band), device_id_type=MESH,
            ).start()

    loads[6].wait()
    high = proj[...].astype(BF16)
    low = (proj[...] - high.astype(F32)).astype(BF16)
    r0 = lax.broadcasted_iota(jnp.int32, (fa, fields), 0) % fields
    r1 = lax.broadcasted_iota(jnp.int32, (fa, fields), 1)
    tile = jnp.where(r0 == r1, 1.0, 0.0).astype(BF16)
    tiled = dot(tile, high).T.astype(BF16)
    for r in (0, 1):
        wrep[r * chans : (r + 1) * chans, r * fa : (r + 1) * fa] = tiled
        wrep[r * chans : (r + 1) * chans, (1 - r) * fa : (2 - r) * fa] = jnp.zeros_like(tiled)
    for i, part in enumerate((high, low)):
        for e in (0, 1):
            at = (2 * i + e) * fields
            drep[at : at + fields, e * chans : (e + 1) * chans] = part
            drep[at : at + fields, (1 - e) * chans : (2 - e) * chans] = jnp.zeros_like(part)
    step_round(0)

    loads[0].wait()

    @pl.when(even)
    def _():
        halo_wait(False, 0)
        halo_wait(False, 1)

    @pl.when(jnp.logical_not(even))
    def _():
        halo_wait(True, 0)
        halo_wait(True, 1)

    convolve(0)
    step_round(1)
    loads[2].wait()
    transform(0)
    direct(0)
    convolve(1)
    step_round(2)
    transform(1)
    direct(1)

    @pl.when(even)
    def _():
        halo_wait(True, 0)

    @pl.when(jnp.logical_not(even))
    def _():
        halo_wait(False, 0)

    for t in range(2, pairs - 1):
        convolve(t)
        transform(t)
        direct(t)

    for i in (3, 4, 5, 7):
        loads[i].wait()
    wtable = (leg[...].astype(F32) * quad[...]).astype(BF16).reshape(mb * degrees, nlat)
    lat_at = lax.broadcasted_iota(jnp.int32, (nlat, nlat), 0)
    place = lax.broadcasted_iota(jnp.int32, (nlat, nlat), 1)
    source = place // 2 % bands
    turn = place // (2 * bands)
    pair_at = jnp.where(source % 2 == 0, pairs - 1 - turn, turn)
    moved = lat_at == source * lat_rows + 2 * pair_at + place % 2
    by_step = dot(wtable, jnp.where(moved, 1.0, 0.0).astype(BF16)).astype(BF16)
    by_step = by_step.reshape(mb, degrees, nlat)
    wearly[...] = by_step[:, :, : nlat - 2 * bands]
    wlate[...] = by_step[:, :, nlat - 2 * bands :]
    for m in range(mb):
        leg_t[m] = leg[m].T
    r0 = lax.broadcasted_iota(jnp.int32, (wide, wide * lat_rows), 0)
    r1 = lax.broadcasted_iota(jnp.int32, (wide, wide * lat_rows), 1)
    gather[...] = jnp.where(r1 // lat_rows == r0, 1.0, 0.0).astype(BF16)
    for i, at in enumerate(lanes):
        width = at.stop - at.start
        own_rows[i, :, :width] = target[:, :, at].astype(F32).reshape(fa, width)
        for a in range(lat_rows):
            rows_of = own_rows[i, pl.ds(a, fields, stride=lat_rows), :]
            observed[a * fields : (a + 1) * fields, at] = rows_of[:, :width]

    for i in range(3, len(rounds)):
        step_round(i)

    send_spec(0, 0)

    @pl.when(even & has_low)
    def _():
        halo(False, 0).wait_send()
        halo(False, 1).wait_send()

    @pl.when(jnp.logical_not(even) & has_high)
    def _():
        halo(True, 0).wait_send()
        halo(True, 1).wait_send()

    neighbour = band ^ 1
    leaves = jnp.where(even, has_low, has_high)
    near_leaves = jnp.where(even, neighbour < bands - 1, neighbour > 0)

    @pl.when(leaves & jnp.logical_not(near_leaves))
    def _():
        pl.semaphore_signal(left_sem.at[0], 1, device_id=(member, neighbour), device_id_type=MESH)

    @pl.when(near_leaves & jnp.logical_not(leaves))
    def _():
        pl.semaphore_wait(left_sem.at[0], 1)

    send_spec(1, pairs - 2)

    final_pair = pair_of(pairs - 1)
    partial[...] = window_sum(final_pair, jnp.where(even, 1, 0), HALF)

    @pl.when(even)
    def _():
        halo_wait(True, 1)

    @pl.when(jnp.logical_not(even))
    def _():
        halo_wait(False, 1)

    mix(final_pair, partial[...] + window_sum(final_pair, jnp.where(even, 0, HALF), 1))
    transform(pairs - 1)
    send_spec(pairs - 1, pairs - 1)
    direct(pairs - 1)

    late = 2 * bands

    def spread_rows(t):
        for source in range(bands):
            q = pairs - 1 - t if source % 2 == 0 else t
            at = (t * bands + source) * 2 * wide
            spread[at : at + 2 * wide, :] = banded[source, q].astype(F32).reshape(2 * wide, chans)

    def sums(m, weights, first, count):
        re = spread[pl.ds(first * wide + m, count, stride=wide), :]
        im = spread[pl.ds(first * wide + mb + m, count, stride=wide), :]
        return dot(weights, jnp.concatenate([re, im], axis=1).astype(BF16))

    wait_spec(0, 0)
    wait_spec(1, pairs - 2)
    for t in range(pairs - 1):
        spread_rows(t)
    for m in range(mb):
        early[m] = sums(m, wearly[m], 0, nlat - late)
    gain_re, gain_im = gain[0], gain[1]
    wait_spec(pairs - 1, pairs - 1)
    spread_rows(pairs - 1)
    for m in range(mb):
        coef = early[m] + sums(m, wlate[m], nlat - late, late)
        c0, c1 = coef[:, :chans], coef[:, chans:]
        real, imag = c0 * gain_re - c1 * gain_im, c0 * gain_im + c1 * gain_re
        filt[m] = jnp.concatenate([real, imag], axis=1).astype(BF16)
    filtw[...] = (
        dot(filt[...].reshape(mb * degrees, 2 * chans), wrep[...])
        .astype(BF16)
        .reshape(mb, degrees, 2 * fa)
    )

    r0 = lax.broadcasted_iota(jnp.int32, (nlat, fa), 0) % lat_rows
    r1 = lax.broadcasted_iota(jnp.int32, (nlat, fa), 1) // fields
    for m in range(mb):
        synth = dot(leg_t[m], filtw[m])
        for r in (0, 1):
            kept = jnp.where(r0 == r1, synth[:, r * fa : (r + 1) * fa], 0.0).astype(BF16)
            masked[:, r * mb + m] = kept.reshape(bands, lat_rows, fa)
    for s in range(bands):
        narrow[s] = dot(gather[...], masked[s].reshape(wide * lat_rows, fa)).astype(BF16)

    me = member * bands + band

    def back(k, s):
        pltpu.make_async_remote_copy(
            narrow.at[s], everyone.at[me], send_sems.at[6], back_sems.at[member],
            device_id=(member ^ k, s), device_id_type=MESH,
        ).start()

    for dest in range(members):

        @pl.loop(0, bands)
        def _(s):
            @pl.when((s != band) | (member != dest))
            def _():
                back(member ^ dest, s)

    pltpu.make_async_copy(narrow.at[band], everyone.at[me], back_sems.at[member]).start()

    def back_wait(j):
        arrived = everyone.at[pl.ds(j * bands, bands)]
        pltpu.make_async_copy(arrived, arrived, back_sems.at[j]).wait()

    def projected(j):
        k = everyone[pl.ds(j * bands, bands)].reshape(bands * wide, fa)
        synth = dot(k, table[...], ((0,), (0,)))
        return (directs[j].astype(F32) + synth).astype(BF16).astype(F32)

    back_wait(member)
    own = projected(member)
    observed[...] = smooth(own - observed[...])
    mine[...] = own
    sent = directs.at[pl.ds(0, members - 1)]
    pltpu.make_async_copy(sent, sent, direct_sems.at[0]).wait()

    @pl.loop(1, members - 1)
    def _(k):
        j = member ^ k
        back_wait(j)
        observed[...] -= smooth(mine[...] - projected(j)) * (1.0 / (members - 1))

    back_wait(member ^ (members - 1))

    @pl.when(even & has_high)
    def _():
        halo(True, 0).wait_send()
        halo(True, 1).wait_send()

    @pl.when(jnp.logical_not(even) & has_low)
    def _():
        halo(False, 0).wait_send()
        halo(False, 1).wait_send()

    sent = banded.at[pl.ds(0, bands - 1)]
    pltpu.make_async_copy(sent, sent, send_sems.at[4]).wait()
    sent = directs.at[pl.ds(0, members - 1)]
    pltpu.make_async_copy(sent, sent, send_sems.at[5]).wait()

    sent = everyone.at[pl.ds(0, members * bands - 1)]
    pltpu.make_async_copy(sent, sent, send_sems.at[6]).wait()


def finish_kernel(
    members, bands, everyone, directs, table, mine, grads, out, tiles, sorted_rows, sems
):
    fields, lat_rows, nlon = out.shape
    last = lax.axis_index("member") ^ (members - 1)
    fa = fields * lat_rows
    k = everyone[pl.ds(last * bands, bands)].reshape(-1, fa).T
    copies = []
    for i, start in enumerate(reversed(range(0, nlon, LANES))):
        width = min(LANES, nlon - start)
        at = slice(start, start + width)
        other = (directs[last, :, at].astype(F32) + dot(k, table[:, at])).astype(BF16)
        term = smooth(mine[:, at] - other.astype(F32)) * (1.0 / (members - 1))
        tiles[i, :, :width] = grads[:, at] - term
        for f in range(fields):
            rows_of = tiles[i, pl.ds(f, lat_rows, stride=fields), :]
            sorted_rows[f, :, at] = rows_of[:, :width]
        part = pl.ds(start, width)
        copies.append(
            pltpu.make_async_copy(sorted_rows.at[:, :, part], out.at[:, :, part], sems.at[i])
        )
        copies[-1].start()
    for copy in copies:
        copy.wait()


def local(state, conv_weight, legendre, quad_weight, spectral_gain, project_weight, target):
    _, lat_rows, nlon, chans = state.shape
    mb, degrees, nlat = legendre.shape
    members, bands = lax.axis_size("member"), lax.axis_size("lat")
    fields = project_weight.shape[1]
    fa, wide, pairs = fields * lat_rows, 2 * mb, lat_rows // 2
    table = dft_table(nlon, mb * bands, bands)
    vmem = pltpu.VMEM
    dma, plain = pltpu.SemaphoreType.DMA, pltpu.SemaphoreType.REGULAR
    results = [
        vmem((members * bands, wide, fa), BF16),
        vmem((members, fa, nlon), BF16),
        vmem(table.shape, BF16),
        vmem((fa, nlon), F32),
        vmem((fa, nlon), F32),
    ]
    kept = sum(
        int(np.prod(r.shape[:-1])) * pl.cdiv(r.shape[-1], LANES) * LANES * jnp.dtype(r.dtype).itemsize
        for r in results
    )
    arrived = pl.pallas_call(
        functools.partial(kernel, members, bands),
        out_shape=results,
        in_specs=[pl.BlockSpec(memory_space=pl.ANY)] * 8,
        out_specs=[pl.BlockSpec(memory_space=pltpu.VMEM)] * 5,
        scratch_shapes=[
            vmem((lat_rows + 2 * HALF, nlon, chans), BF16),
            vmem(conv_weight.shape, BF16),
            vmem(legendre.shape, BF16),
            vmem((1, nlat), F32),
            vmem(spectral_gain.shape, F32),
            vmem((fields, chans), F32),
            vmem(target.shape, BF16),
            vmem(((2 * HALF + 2) * chans, 2 * chans), BF16),
            vmem((nlon, 2 * chans), F32),
            vmem((pairs, nlon, 2 * chans), BF16),
            vmem((bands, pairs, 2, wide, chans), BF16),
            vmem((bands, pairs, 2, wide, chans), BF16),
            vmem((nlat * wide, chans), F32),
            vmem((mb, degrees, nlat - 2 * bands), BF16),
            vmem((mb, degrees, 2 * bands), BF16),
            vmem((mb, degrees, 2 * chans), F32),
            vmem((mb, nlat, degrees), BF16),
            vmem((wide, wide * lat_rows), BF16),
            vmem((bands, wide, lat_rows, fa), BF16),
            vmem((mb, degrees, 2 * chans), BF16),
            vmem((mb, degrees, 2 * fa), BF16),
            vmem((2 * chans, 2 * fa), BF16),
            vmem((4 * fields, 2 * chans), BF16),
            vmem((bands, wide, fa), BF16),
            vmem((pl.cdiv(nlon, LANES), fa, LANES), F32),
            dma((8,)),
            dma((4,)),
            dma((7,)),
            dma((pairs,)),
            dma((1,)),
            dma((members,)),
            plain((max(1, (bands - 1).bit_length()),)),
            plain((max(1, (members - 1).bit_length()),)),
            plain((1,)),
        ],
        compiler_params=pltpu.CompilerParams(
            collective_id=0,
            has_side_effects=True,
            vmem_limit_bytes=VMEM_BYTES - kept - 2 * 1024 * 1024,
        ),
    )(
        state,
        conv_weight,
        legendre,
        quad_weight.reshape(1, nlat),
        spectral_gain,
        project_weight.T,
        target,
        table,
    )
    tiles = pl.cdiv(nlon, LANES)
    out = pl.pallas_call(
        functools.partial(finish_kernel, members, bands),
        out_shape=jax.ShapeDtypeStruct((fields, lat_rows, nlon), F32),
        in_specs=[pl.BlockSpec(memory_space=pltpu.VMEM)] * 5,
        out_specs=pl.BlockSpec(memory_space=pl.ANY),
        scratch_shapes=[
            vmem((tiles, fa, LANES), F32),
            vmem((fields, lat_rows, nlon), F32),
            dma((tiles,)),
        ],
        compiler_params=pltpu.CompilerParams(vmem_limit_bytes=16 * 1024 * 1024),
    )(*arrived)
    return out[None]


def solution(mesh):
    return jax.shard_map(
        local,
        mesh=mesh,
        in_specs=(
            P("member", "lat", None, None),
            P(),
            P("lat", None, None),
            P(),
            P(),
            P(),
            P(None, "lat", None),
        ),
        out_specs=P("member", None, "lat", None),
        check_vma=False,
    )
```

```python
import functools
import jax
import jax.numpy as jnp
import numpy as np
from jax import lax
from jax.experimental import pallas as pl
from jax.experimental.pallas import tpu as pltpu
from jax.sharding import PartitionSpec as P

MESH = pl.DeviceIdType.MESH
HALF = 4
LANES = 128
VMEM_BYTES = 67043328
F32 = jnp.float32
BF16 = jnp.bfloat16


def dft_table(nlon, modes, bands):
    phase = np.arange(nlon)[:, None] * np.arange(modes)[None, :] % nlon
    angle = phase * (2.0 * np.pi / nlon)
    table = np.stack([np.cos(angle), -np.sin(angle)], axis=1) / np.sqrt(nlon)
    table = table.reshape(nlon, 2, bands, modes // bands).swapaxes(1, 2)
    return jnp.asarray(table.reshape(nlon, 2 * modes).T.astype(np.float32), BF16)


def dot(a, b, contract=((1,), (0,))):
    return lax.dot_general(a, b, (contract, ((), ())), preferred_element_type=F32)


def smooth(diff):
    return diff * lax.rsqrt(diff * diff + 0.25)


def kernel(
    members,
    bands,
    state,
    conv_hbm,
    leg_hbm,
    quad_hbm,
    gain_hbm,
    proj_hbm,
    target_hbm,
    table_hbm,
    everyone,
    directs,
    table,
    mine,
    observed,
    rows,
    conv_w,
    leg,
    quad,
    gain,
    proj,
    target,
    toeplitz,
    partial,
    mixed,
    spec,
    banded,
    spread,
    wearly,
    wlate,
    early,
    leg_t,
    gather,
    masked,
    filt,
    filtw,
    wrep,
    drep,
    narrow,
    own_rows,
    load_sems,
    halo_sems,
    send_sems,
    spec_sems,
    direct_sems,
    back_sems,
    lat_sems,
    member_sems,
    left_sem,
):
    member, band = lax.axis_index("member"), lax.axis_index("lat")
    _, lat_rows, nlon, chans = state.shape
    pairs = lat_rows // 2
    nlat = bands * lat_rows
    mb, degrees = leg.shape[0], leg.shape[1]
    wide = 2 * mb
    fields = proj.shape[0]
    fa = fields * lat_rows
    lanes = [slice(i, min(i + LANES, nlon)) for i in range(0, nlon, LANES)]
    has_low, has_high = band > 0, band < bands - 1

    barrier = pltpu.get_barrier_semaphore()
    hops = [1 << i for i in range((members - 1).bit_length())]

    def greet_lat(sem, dist):
        @pl.when(band >= dist)
        def _():
            pl.semaphore_signal(sem, 1, device_id=(member, band - dist), device_id_type=MESH)

        @pl.when(band + dist < bands)
        def _():
            pl.semaphore_signal(sem, 1, device_id=(member, band + dist), device_id_type=MESH)

    def count_lat(dist):
        return (band >= dist).astype(jnp.int32) + (band + dist < bands).astype(jnp.int32)

    greet_lat(barrier, 1)
    for hop in hops:
        pl.semaphore_signal(barrier, 1, device_id=(member ^ hop, band), device_id_type=MESH)
    loads = [
        (state.at[0], rows.at[pl.ds(HALF, lat_rows)]),
        (conv_hbm, conv_w),
        (table_hbm, table),
        (leg_hbm, leg),
        (quad_hbm, quad),
        (gain_hbm, gain),
        (proj_hbm, proj),
        (target_hbm, target),
    ]
    loads = [pltpu.make_async_copy(a, b, load_sems.at[i]) for i, (a, b) in enumerate(loads)]
    for copy in loads:
        copy.start()
    pl.semaphore_wait(barrier, count_lat(1) + len(hops))

    rounds = []
    for i, hop in enumerate(hops[1:]):
        rounds.append((member_sems.at[i], hop, None))
    known = 1
    while known < bands - 1:
        rounds.append((lat_sems.at[len(rounds) - len(hops) + 1], None, known))
        known *= 2

    def round_signal(i):
        if i < len(rounds):
            sem, hop, dist = rounds[i]
            if hop is None:
                greet_lat(sem, dist)
            else:
                pl.semaphore_signal(sem, 1, device_id=(member ^ hop, band), device_id_type=MESH)

    def step_round(i):
        if i < len(rounds):
            sem, hop, dist = rounds[i]
            pl.semaphore_wait(sem, 1 if hop is not None else count_lat(dist))
            round_signal(i + 1)

    round_signal(0)

    def halo(up, far):
        if up:
            src = lat_rows - 2 - 2 * far
            dst = HALF - 2 - 2 * far
            peer = band + 1
        else:
            src = 2 * far
            dst = HALF + lat_rows + 2 * far
            peer = band - 1
        sem = 2 * (0 if up else 1) + far
        return pltpu.make_async_remote_copy(
            state.at[0, pl.ds(src, 2)],
            rows.at[pl.ds(dst, 2)],
            send_sems.at[sem],
            halo_sems.at[sem],
            device_id=(member, peer),
            device_id_type=MESH,
        )

    even = band % 2 == 0

    @pl.when(even & has_low)
    def _():
        halo(False, 0).start()
        halo(False, 1).start()

    @pl.when(has_high)
    def _():
        halo(True, 0).start()
        halo(True, 1).start()

    @pl.when(jnp.logical_not(even) & has_low)
    def _():
        halo(False, 0).start()
        halo(False, 1).start()

    @pl.when(jnp.logical_not(has_low))
    def _():
        rows[0:HALF] = jnp.zeros((HALF, nlon, chans), BF16)

    @pl.when(jnp.logical_not(has_high))
    def _():
        rows[HALF + lat_rows :] = jnp.zeros((HALF, nlon, chans), BF16)

    def halo_wait(low, far):
        at = HALF - 2 - 2 * far if low else HALF + lat_rows + 2 * far
        sem = 2 * (0 if low else 1) + far

        @pl.when(has_low if low else has_high)
        def _():
            part = rows.at[pl.ds(at, 2)]
            pltpu.make_async_copy(part, part, halo_sems.at[sem]).wait()

    loads[1].wait()
    taps = conv_w.shape[0]
    for d in range(HALF + 1):
        for e in (0, 1):
            for f in (0, 1):
                tap = 2 * d + e - f
                w = conv_w[tap] if 0 <= tap < taps else jnp.zeros((chans, chans), BF16)
                at = (2 * d + e) * chans
                toeplitz[at : at + chans, f * chans : (f + 1) * chans] = w
    def pair_of(t):
        return jnp.where(even, pairs - 1 - t, t)

    def mix(p, conv):
        own = jnp.concatenate([rows[2 * p + HALF], rows[2 * p + HALF + 1]], axis=1)
        half = conv * 0.5
        mixed[p] = (own.astype(F32) + half + half * jnp.tanh(half)).astype(BF16)

    def window_sum(p, first, count):
        window = [rows[2 * (p + first) + j] for j in range(2 * count)]
        at = pl.ds(pl.multiple_of(first * 2 * chans, 2 * chans), count * 2 * chans)
        return dot(jnp.concatenate(window, axis=1), toeplitz[at, :])

    def convolve(t):
        p = pair_of(t)
        mix(p, window_sum(p, 0, HALF + 1))

    def transform(t):
        p = pair_of(t)
        s = dot(table[...], mixed[p]).astype(BF16)
        for e in (0, 1):
            spec[:, p, e] = s[:, e * chans : (e + 1) * chans].reshape(bands, wide, chans)

    def send_spec(first, last):
        at = pl.ds(jnp.where(even, pairs - 1 - last, first), last - first + 1)
        arrival = spec_sems.at[first]

        def to(peer):
            pltpu.make_async_remote_copy(
                spec.at[peer, at], banded.at[band, at], send_sems.at[4], arrival,
                device_id=(member, peer), device_id_type=MESH,
            ).start()

        for dist in range(bands - 1, 0, -1):

            @pl.when(band >= dist)
            def _():
                to(band - dist)

        for dist in range(bands - 1, 0, -1):

            @pl.when(band + dist < bands)
            def _():
                to(band + dist)

        pltpu.make_async_copy(spec.at[band, at], banded.at[band, at], arrival).start()

    def wait_spec(first, last):
        part = banded.at[:, pl.ds(first, last - first + 1)]
        pltpu.make_async_copy(part, part, spec_sems.at[first]).wait()

    def direct(t):
        p = pair_of(t)
        fine = dot(drep[...], mixed[p], ((1,), (1,)))
        half = 2 * fields
        at = pl.ds(p * half, half)
        directs[member, at] = (fine[:half] + fine[half:]).astype(BF16)

        @pl.loop(1, members)
        def _(k):
            part = directs.at[member, at]
            pltpu.make_async_remote_copy(
                part, part, send_sems.at[5], direct_sems.at[0],
                device_id=(member ^ k, band), device_id_type=MESH,
            ).start()

    loads[6].wait()
    high = proj[...].astype(BF16)
    low = (proj[...] - high.astype(F32)).astype(BF16)
    r0 = lax.broadcasted_iota(jnp.int32, (fa, fields), 0) % fields
    r1 = lax.broadcasted_iota(jnp.int32, (fa, fields), 1)
    tile = jnp.where(r0 == r1, 1.0, 0.0).astype(BF16)
    tiled = dot(tile, high).T.astype(BF16)
    for r in (0, 1):
        wrep[r * chans : (r + 1) * chans, r * fa : (r + 1) * fa] = tiled
        wrep[r * chans : (r + 1) * chans, (1 - r) * fa : (2 - r) * fa] = jnp.zeros_like(tiled)
    for i, part in enumerate((high, low)):
        for e in (0, 1):
            at = (2 * i + e) * fields
            drep[at : at + fields, e * chans : (e + 1) * chans] = part
            drep[at : at + fields, (1 - e) * chans : (2 - e) * chans] = jnp.zeros_like(part)
    step_round(0)

    loads[0].wait()

    @pl.when(even)
    def _():
        halo_wait(False, 0)
        halo_wait(False, 1)

    @pl.when(jnp.logical_not(even))
    def _():
        halo_wait(True, 0)
        halo_wait(True, 1)

    convolve(0)
    step_round(1)
    loads[2].wait()
    transform(0)
    direct(0)
    convolve(1)
    step_round(2)
    transform(1)
    direct(1)

    @pl.when(even)
    def _():
        halo_wait(True, 0)

    @pl.when(jnp.logical_not(even))
    def _():
        halo_wait(False, 0)

    for t in range(2, pairs - 1):
        convolve(t)
        transform(t)
        direct(t)

    for i in (3, 4, 5, 7):
        loads[i].wait()
    wtable = (leg[...].astype(F32) * quad[...]).astype(BF16).reshape(mb * degrees, nlat)
    lat_at = lax.broadcasted_iota(jnp.int32, (nlat, nlat), 0)
    place = lax.broadcasted_iota(jnp.int32, (nlat, nlat), 1)
    source = place // 2 % bands
    turn = place // (2 * bands)
    pair_at = jnp.where(source % 2 == 0, pairs - 1 - turn, turn)
    moved = lat_at == source * lat_rows + 2 * pair_at + place % 2
    by_step = dot(wtable, jnp.where(moved, 1.0, 0.0).astype(BF16)).astype(BF16)
    by_step = by_step.reshape(mb, degrees, nlat)
    wearly[...] = by_step[:, :, : nlat - 2 * bands]
    wlate[...] = by_step[:, :, nlat - 2 * bands :]
    for m in range(mb):
        leg_t[m] = leg[m].T
    r0 = lax.broadcasted_iota(jnp.int32, (wide, wide * lat_rows), 0)
    r1 = lax.broadcasted_iota(jnp.int32, (wide, wide * lat_rows), 1)
    gather[...] = jnp.where(r1 // lat_rows == r0, 1.0, 0.0).astype(BF16)
    for i, at in enumerate(lanes):
        width = at.stop - at.start
        own_rows[i, :, :width] = target[:, :, at].astype(F32).reshape(fa, width)
        for a in range(lat_rows):
            rows_of = own_rows[i, pl.ds(a, fields, stride=lat_rows), :]
            observed[a * fields : (a + 1) * fields, at] = rows_of[:, :width]

    for i in range(3, len(rounds)):
        step_round(i)

    send_spec(0, 0)

    @pl.when(even & has_low)
    def _():
        halo(False, 0).wait_send()
        halo(False, 1).wait_send()

    @pl.when(jnp.logical_not(even) & has_high)
    def _():
        halo(True, 0).wait_send()
        halo(True, 1).wait_send()

    neighbour = band ^ 1
    leaves = jnp.where(even, has_low, has_high)
    near_leaves = jnp.where(even, neighbour < bands - 1, neighbour > 0)

    @pl.when(leaves & jnp.logical_not(near_leaves))
    def _():
        pl.semaphore_signal(left_sem.at[0], 1, device_id=(member, neighbour), device_id_type=MESH)

    @pl.when(near_leaves & jnp.logical_not(leaves))
    def _():
        pl.semaphore_wait(left_sem.at[0], 1)

    send_spec(1, pairs - 2)

    final_pair = pair_of(pairs - 1)
    partial[...] = window_sum(final_pair, jnp.where(even, 1, 0), HALF)

    @pl.when(even)
    def _():
        halo_wait(True, 1)

    @pl.when(jnp.logical_not(even))
    def _():
        halo_wait(False, 1)

    mix(final_pair, partial[...] + window_sum(final_pair, jnp.where(even, 0, HALF), 1))
    transform(pairs - 1)
    send_spec(pairs - 1, pairs - 1)
    direct(pairs - 1)

    late = 2 * bands

    def spread_rows(t):
        for source in range(bands):
            q = pairs - 1 - t if source % 2 == 0 else t
            at = (t * bands + source) * 2 * wide
            spread[at : at + 2 * wide, :] = banded[source, q].astype(F32).reshape(2 * wide, chans)

    def sums(m, weights, first, count):
        re = spread[pl.ds(first * wide + m, count, stride=wide), :]
        im = spread[pl.ds(first * wide + mb + m, count, stride=wide), :]
        return dot(weights, jnp.concatenate([re, im], axis=1).astype(BF16))

    wait_spec(0, 0)
    wait_spec(1, pairs - 2)
    for t in range(pairs - 1):
        spread_rows(t)
    for m in range(mb):
        early[m] = sums(m, wearly[m], 0, nlat - late)
    gain_re, gain_im = gain[0], gain[1]
    wait_spec(pairs - 1, pairs - 1)
    spread_rows(pairs - 1)
    for m in range(mb):
        coef = early[m] + sums(m, wlate[m], nlat - late, late)
        c0, c1 = coef[:, :chans], coef[:, chans:]
        real, imag = c0 * gain_re - c1 * gain_im, c0 * gain_im + c1 * gain_re
        filt[m] = jnp.concatenate([real, imag], axis=1).astype(BF16)
    filtw[...] = (
        dot(filt[...].reshape(mb * degrees, 2 * chans), wrep[...])
        .astype(BF16)
        .reshape(mb, degrees, 2 * fa)
    )

    r0 = lax.broadcasted_iota(jnp.int32, (nlat, fa), 0) % lat_rows
    r1 = lax.broadcasted_iota(jnp.int32, (nlat, fa), 1) // fields
    for m in range(mb):
        synth = dot(leg_t[m], filtw[m])
        for r in (0, 1):
            kept = jnp.where(r0 == r1, synth[:, r * fa : (r + 1) * fa], 0.0).astype(BF16)
            masked[:, r * mb + m] = kept.reshape(bands, lat_rows, fa)
    for s in range(bands):
        narrow[s] = dot(gather[...], masked[s].reshape(wide * lat_rows, fa)).astype(BF16)

    me = member * bands + band

    def back(k, s):
        pltpu.make_async_remote_copy(
            narrow.at[s], everyone.at[me], send_sems.at[6], back_sems.at[member],
            device_id=(member ^ k, s), device_id_type=MESH,
        ).start()

    for dest in range(members):

        @pl.loop(0, bands)
        def _(s):
            @pl.when((s != band) | (member != dest))
            def _():
                back(member ^ dest, s)

    pltpu.make_async_copy(narrow.at[band], everyone.at[me], back_sems.at[member]).start()

    def back_wait(j):
        arrived = everyone.at[pl.ds(j * bands, bands)]
        pltpu.make_async_copy(arrived, arrived, back_sems.at[j]).wait()

    def projected(j):
        k = everyone[pl.ds(j * bands, bands)].reshape(bands * wide, fa)
        synth = dot(k, table[...], ((0,), (0,)))
        return (directs[j].astype(F32) + synth).astype(BF16).astype(F32)

    back_wait(member)
    own = projected(member)
    observed[...] = smooth(own - observed[...])
    mine[...] = own
    sent = directs.at[pl.ds(0, members - 1)]
    pltpu.make_async_copy(sent, sent, direct_sems.at[0]).wait()

    @pl.loop(1, members - 1)
    def _(k):
        j = member ^ k
        back_wait(j)
        observed[...] -= smooth(mine[...] - projected(j)) * (1.0 / (members - 1))

    back_wait(member ^ (members - 1))

    @pl.when(even & has_high)
    def _():
        halo(True, 0).wait_send()
        halo(True, 1).wait_send()

    @pl.when(jnp.logical_not(even) & has_low)
    def _():
        halo(False, 0).wait_send()
        halo(False, 1).wait_send()

    sent = banded.at[pl.ds(0, bands - 1)]
    pltpu.make_async_copy(sent, sent, send_sems.at[4]).wait()
    sent = directs.at[pl.ds(0, members - 1)]
    pltpu.make_async_copy(sent, sent, send_sems.at[5]).wait()

    sent = everyone.at[pl.ds(0, members * bands - 1)]
    pltpu.make_async_copy(sent, sent, send_sems.at[6]).wait()


def finish_kernel(
    members, bands, everyone, directs, table, mine, grads, out, tiles, sorted_rows, sems
):
    fields, lat_rows, nlon = out.shape
    last = lax.axis_index("member") ^ (members - 1)
    fa = fields * lat_rows
    k = everyone[pl.ds(last * bands, bands)].reshape(-1, fa).T
    copies = []
    for i, start in enumerate(reversed(range(0, nlon, LANES))):
        width = min(LANES, nlon - start)
        at = slice(start, start + width)
        other = (directs[last, :, at].astype(F32) + dot(k, table[:, at])).astype(BF16)
        term = smooth(mine[:, at] - other.astype(F32)) * (1.0 / (members - 1))
        tiles[i, :, :width] = grads[:, at] - term
        for f in range(fields):
            rows_of = tiles[i, pl.ds(f, lat_rows, stride=fields), :]
            sorted_rows[f, :, at] = rows_of[:, :width]
        part = pl.ds(start, width)
        copies.append(
            pltpu.make_async_copy(sorted_rows.at[:, :, part], out.at[:, :, part], sems.at[i])
        )
        copies[-1].start()
    for copy in copies:
        copy.wait()


def local(state, conv_weight, legendre, quad_weight, spectral_gain, project_weight, target):
    _, lat_rows, nlon, chans = state.shape
    mb, degrees, nlat = legendre.shape
    members, bands = lax.axis_size("member"), lax.axis_size("lat")
    assert members & (members - 1) == 0 and bands % 2 == 0
    assert lat_rows % 2 == 0 and lat_rows >= 6
    fields = project_weight.shape[1]
    fa, wide, pairs = fields * lat_rows, 2 * mb, lat_rows // 2
    table = dft_table(nlon, mb * bands, bands)
    vmem = pltpu.VMEM
    dma, plain = pltpu.SemaphoreType.DMA, pltpu.SemaphoreType.REGULAR
    results = [
        vmem((members * bands, wide, fa), BF16),
        vmem((members, fa, nlon), BF16),
        vmem(table.shape, BF16),
        vmem((fa, nlon), F32),
        vmem((fa, nlon), F32),
    ]
    kept = sum(
        int(np.prod(r.shape[:-1])) * pl.cdiv(r.shape[-1], LANES) * LANES * jnp.dtype(r.dtype).itemsize
        for r in results
    )
    arrived = pl.pallas_call(
        functools.partial(kernel, members, bands),
        out_shape=results,
        in_specs=[pl.BlockSpec(memory_space=pl.ANY)] * 8,
        out_specs=[pl.BlockSpec(memory_space=pltpu.VMEM)] * 5,
        scratch_shapes=[
            vmem((lat_rows + 2 * HALF, nlon, chans), BF16),
            vmem(conv_weight.shape, BF16),
            vmem(legendre.shape, BF16),
            vmem((1, nlat), F32),
            vmem(spectral_gain.shape, F32),
            vmem((fields, chans), F32),
            vmem(target.shape, BF16),
            vmem(((2 * HALF + 2) * chans, 2 * chans), BF16),
            vmem((nlon, 2 * chans), F32),
            vmem((pairs, nlon, 2 * chans), BF16),
            vmem((bands, pairs, 2, wide, chans), BF16),
            vmem((bands, pairs, 2, wide, chans), BF16),
            vmem((nlat * wide, chans), F32),
            vmem((mb, degrees, nlat - 2 * bands), BF16),
            vmem((mb, degrees, 2 * bands), BF16),
            vmem((mb, degrees, 2 * chans), F32),
            vmem((mb, nlat, degrees), BF16),
            vmem((wide, wide * lat_rows), BF16),
            vmem((bands, wide, lat_rows, fa), BF16),
            vmem((mb, degrees, 2 * chans), BF16),
            vmem((mb, degrees, 2 * fa), BF16),
            vmem((2 * chans, 2 * fa), BF16),
            vmem((4 * fields, 2 * chans), BF16),
            vmem((bands, wide, fa), BF16),
            vmem((pl.cdiv(nlon, LANES), fa, LANES), F32),
            dma((8,)),
            dma((4,)),
            dma((7,)),
            dma((pairs,)),
            dma((1,)),
            dma((members,)),
            plain((max(1, (bands - 1).bit_length()),)),
            plain((max(1, (members - 1).bit_length()),)),
            plain((1,)),
        ],
        compiler_params=pltpu.CompilerParams(
            collective_id=0,
            has_side_effects=True,
            vmem_limit_bytes=VMEM_BYTES - kept - 2 * 1024 * 1024,
        ),
    )(
        state,
        conv_weight,
        legendre,
        quad_weight.reshape(1, nlat),
        spectral_gain,
        project_weight.T,
        target,
        table,
    )
    tiles = pl.cdiv(nlon, LANES)
    out = pl.pallas_call(
        functools.partial(finish_kernel, members, bands),
        out_shape=jax.ShapeDtypeStruct((fields, lat_rows, nlon), F32),
        in_specs=[pl.BlockSpec(memory_space=pltpu.VMEM)] * 5,
        out_specs=pl.BlockSpec(memory_space=pl.ANY),
        scratch_shapes=[
            vmem((tiles, fa, LANES), F32),
            vmem((fields, lat_rows, nlon), F32),
            dma((tiles,)),
        ],
        compiler_params=pltpu.CompilerParams(vmem_limit_bytes=16 * 1024 * 1024),
    )(*arrived)
    return out[None]


def solution(mesh):
    return jax.shard_map(
        local,
        mesh=mesh,
        in_specs=(
            P("member", "lat", None, None),
            P(),
            P("lat", None, None),
            P(),
            P(),
            P(),
            P(None, "lat", None),
        ),
        out_specs=P("member", None, "lat", None),
        check_vma=False,
    )
```
